32 devices in a mesh: shard: 4 (over y, x), context: 2 (over core), tensor: 4 (over z).
Axes of the slice: x: 2, y: 2, z: 4, core: 2. Of those that a mesh axis runs over, the one named last changes fastest.
Arguments:
- inputs: bfloat16 [4, 1024, 1024], P('shard', 'context'), may hold values from -6 to 6
- cotangent: bfloat16 [4, 1024, 1024], P('shard', 'context'), may hold values from -6 to 6
- segments: int32 [4, 1024], P('shard'), may hold values from 0 to 3, never falling along the last dimension, each value on 1 to 800 neighbouring positions
- buckets: int32 [2047], replicated, may hold values from 0 to 511, as said below
- w_query: bfloat16 [1024, 1024], P(('shard', 'context'), 'tensor'), may hold values from -0.1875 to 0.1875
- w_key: bfloat16 [1024, 1024], P(('shard', 'context'), 'tensor'), may hold values from -0.1875 to 0.1875
- w_value: bfloat16 [1024, 1024], P(('shard', 'context'), 'tensor'), may hold values from -0.1875 to 0.1875
- w_output: bfloat16 [1024, 1024], P('tensor', ('shard', 'context')), may hold values from -3 to 3
- w_up: bfloat16 [1024, 4096], P(('shard', 'context'), 'tensor'), may hold values from -0.1875 to 0.1875
- w_down: bfloat16 [4096, 1024], P('tensor', ('shard', 'context')), may hold values from -0.09375 to 0.09375
- positions: bfloat16 [512, 1024], P(None, ('shard', 'context')), may hold values from -6 to 6
- gain_attn: bfloat16 [1024], P(('shard', 'context')), may hold values from 0.5 to 1.5
- bias_attn: bfloat16 [1024], P(('shard', 'context')), may hold values from -4 to 4
- gain_ffn: bfloat16 [1024], P(('shard', 'context')), may hold values from 0.5 to 1.5
- bias_ffn: bfloat16 [1024], P(('shard', 'context')), may hold values from -4 to 4
Outputs:
- outputs: bfloat16 [4, 1024, 1024], P('shard', 'context')
- grad_inputs: bfloat16 [4, 1024, 1024], P('shard', 'context')
- grad_query: float32 [1024, 1024], P(('shard', 'context'), 'tensor')
- grad_key: float32 [1024, 1024], P(('shard', 'context'), 'tensor')
- grad_value: float32 [1024, 1024], P(('shard', 'context'), 'tensor')
- grad_output: float32 [1024, 1024], P('tensor', ('shard', 'context'))
- grad_up: float32 [1024, 4096], P(('shard', 'context'), 'tensor')
- grad_down: float32 [4096, 1024], P('tensor', ('shard', 'context'))
- grad_positions: float32 [512, 1024], P(None, ('shard', 'context'))
- grad_gain_attn: float32 [1024], P(('shard', 'context'))
- grad_bias_attn: float32 [1024], P(('shard', 'context'))
- grad_gain_ffn: float32 [1024], P(('shard', 'context'))
- grad_bias_ffn: float32 [1024], P(('shard', 'context'))
The draws below stay inside these ranges and needn't reach their ends.
Inputs may be any that keep to these rules, and one draw needn't show every extreme that they name: buckets[d + 1023] is the bucket of the distance d from key to query; it is 256 at d = 0, never falls as d rises, and equals d + 256 for small distances. `segments`: within a sequence document numbers never fall; each document has at least one token.
All inputs are finite; a program needn't handle non-finite values.
Results may differ from the reference program's by a relative error of at most 0.02.
Values may be sent and summed in bfloat16 or wider, within the bound.
A program may use at most 192 MiB of HBM per device.

```python
import math
import jax
import jax.numpy as jnp
import numpy as np
from jax import lax

D = 1024
H = 16
HD = 64
FF = 4096
SPAN = 256
LEN = 1024
SEQS = 4


def draw_buckets(key, part):
    coin_flips = jax.random.randint(key, (LEN - 1,), 0, 2)
    distance = jnp.arange(1, LEN, dtype=jnp.int32)
    forced = (distance <= SPAN // 2) | (distance >= LEN - SPAN)
    increments = jnp.where(forced, 1, coin_flips).astype(jnp.int32)
    magnitude = jnp.minimum(jnp.cumsum(increments), SPAN).astype(jnp.int32)
    forward_side = jnp.minimum(SPAN + magnitude, 2 * SPAN - 1)
    behind = SPAN - magnitude
    middle = jnp.full((1,), SPAN, jnp.int32)
    return jnp.concatenate([behind[::-1], middle, forward_side]).astype(jnp.int32)


def shard_levels(stream_key, shape, split, low, high):
    gain, own = 1.0, jax.random.fold_in(stream_key, 6)
    for position, blocks in split:
        heights = jnp.exp(jax.random.uniform(jax.random.fold_in(own, position), (blocks,), jnp.float32, low / len(split), high / len(split)))
        gain = gain * jnp.repeat(heights, shape[position] // blocks).reshape([-1 if axis == position else 1 for axis in range(len(shape))])
    return gain


def length_profile(amount, total, reach, slope):
    weights = [(1 << 20) // math.isqrt(grade ** slope) + 1 for grade in range(2, amount + 1)]
    spare, holding = total - reach - (amount - 1), [1] * (amount - 1)
    while spare > 0:
        free = [i for i in range(amount - 1) if holding[i] < reach]
        whole, left = sum([weights[i] for i in free]), spare
        for i in free:
            more = min(reach - holding[i], max(1, left * weights[i] // whole), spare)
            holding[i] = holding[i] + more
            spare = spare - more
    return np.array([reach] + holding)


def ragged(rng, number_of, total, bound, slope):
    if number_of == 2:
        one = jax.random.randint(rng, (), max(1, total - bound), min(bound, total - 1) + 1)
        return jnp.stack([one, total - one])
    tallies = jnp.asarray(length_profile(number_of, total, bound, slope), jnp.int32)
    twos = (number_of - 1) // 2
    source_of, taker = tallies[1:1 + 2 * twos:2], tallies[2:2 + 2 * twos:2]
    slack = jnp.minimum(source_of - 1, bound - taker)
    passed = jax.random.randint(jax.random.fold_in(rng, 1), (twos,), 0, 1 << 20) % (slack + 1)
    tallies = tallies.at[1:1 + 2 * twos:2].set(source_of - passed).at[2:2 + 2 * twos:2].set(taker + passed)
    return tallies[jax.random.permutation(jax.random.fold_in(rng, 2), number_of)]


def gaussian(key, shape, scale, limit, pieces=(), held_as=jnp.bfloat16):
    values = jax.random.normal(key, shape, jnp.float32) * scale
    if len(pieces) > 0:
        values = shard_levels(key, shape, pieces, -0.22, 0.18) * values
    return jnp.clip(values, min=-limit, max=limit).astype(held_as)


def setup_inputs(seed: int = 0) -> dict:
    keys = jax.random.split(jax.random.key(seed), 16)
    inputs = gaussian(keys[0], (SEQS, LEN, D), 1.0, 6.0, ((0, 4), (1, 2)))
    cotangent = gaussian(keys[1], (SEQS, LEN, D), 1.0, 6.0, ((0, 4), (1, 2)))
    segments = jax.vmap(lambda own: jnp.searchsorted(jnp.cumsum(ragged(own, 4, LEN, LEN * 25 // 32, 1)), jnp.arange(LEN), side="right"))(jax.random.split(keys[2], SEQS)).reshape((SEQS, LEN)).astype(jnp.int32)
    buckets = draw_buckets(jax.random.fold_in(keys[15], 71), 0)
    w_query = gaussian(keys[4], (D, D), D ** -0.5, 0.1875, ((0, 8), (1, 4)))
    w_key = gaussian(keys[5], (D, D), D ** -0.5, 0.1875, ((0, 8), (1, 4)))
    w_value = gaussian(keys[6], (D, D), D ** -0.5, 0.1875, ((0, 8), (1, 4)))
    w_output = gaussian(keys[7], (D, D), (max(1, D // 256)) ** -0.5, 3.0, ((0, 4), (1, 8)))
    w_up = gaussian(keys[8], (D, FF), D ** -0.5, 0.1875, ((0, 8), (1, 4)))
    w_down = gaussian(keys[9], (FF, D), FF ** -0.5, 0.09375, ((0, 4), (1, 8)))
    positions = gaussian(keys[10], (2 * SPAN, D), 1.0, 6.0, ((1, 8),))
    gain_attn = jnp.clip(1.0 + 0.1 * jax.random.normal(keys[11], (D,), jnp.float32), 0.5, 1.5).astype(jnp.bfloat16)
    bias_attn = gaussian(keys[12], (D,), 0.3, 4.0, ((0, 8),))
    gain_ffn = jnp.clip(1.0 + 0.1 * jax.random.normal(keys[13], (D,), jnp.float32), 0.5, 1.5).astype(jnp.bfloat16)
    bias_ffn = gaussian(keys[14], (D,), 0.3, 4.0, ((0, 8),))
    return dict(inputs=inputs, cotangent=cotangent, segments=segments, buckets=buckets, w_query=w_query, w_key=w_key, w_value=w_value, w_output=w_output, w_up=w_up, w_down=w_down, positions=positions, gain_attn=gain_attn, bias_attn=bias_attn, gain_ffn=gain_ffn, bias_ffn=bias_ffn)


eps_norm = 1e-06
neg_fill = -1000000000.0
exact_precision_option = lax.Precision.HIGHEST

@jax.custom_vjp
def low(v):
    return lax.optimization_barrier(v.astype(jnp.bfloat16)).astype(jnp.float32)

@jax.custom_vjp
def low_back(v):
    return v

def low_keep(v):
    return (low(v), None)

def low_pass(kept, grad):
    return (grad,)

def back_keep(v):
    return (v, None)

def back_low(kept, grad):
    return (low(grad),)
low.defvjp(low_keep, low_pass)
low_back.defvjp(back_keep, back_low)

def layer_norm(values, gain_row, shift_row):
    center = values - lax.optimization_barrier(jnp.mean(values, axis=-1, keepdims=True))
    spread = lax.optimization_barrier(jnp.mean(center * center, axis=-1, keepdims=True))
    return center * lax.rsqrt(spread + eps_norm) * gain_row + shift_row

def project(matrix, weight):
    return jnp.dot(matrix, weight, precision=exact_precision_option)

def forward(inputs, w_query, w_key, w_value, w_output, w_up, w_down, positions, gain_attn, bias_attn, gain_ffn, bias_ffn, segments, buckets):
    count_seq, length, model_width = inputs.shape
    flat_rows = inputs.reshape(-1, model_width)

    def split_into_heads(weight):
        return low(low_back(project(flat_rows, weight))).reshape(count_seq, length, H, HD)
    queries = split_into_heads(w_query)
    keys_all = split_into_heads(w_key)
    values_all = split_into_heads(w_value)
    position_key_rows = low(project(positions, w_key)).reshape(2 * SPAN, H, HD)
    pos_query = low(project(positions, w_query)).reshape(2 * SPAN, H, HD)
    places = jnp.arange(length, dtype=jnp.int32)
    offsets = places[:, None] - places[None, :] + (length - 1)
    c2p_index = jnp.broadcast_to(buckets[offsets][None], (H, length, length))
    score_scale = 1.0 / jnp.sqrt(jnp.float32(3 * HD))

    def attend(running, block_items):
        query_scaled, key_s, value_s, seg_s = block_items
        content = jnp.einsum('ihd,jhd->hij', query_scaled, key_s, precision=exact_precision_option)
        query_position_rows = jnp.einsum('ocy,xcy->cox', query_scaled, position_key_rows, precision=exact_precision_option)
        to_pos = jnp.take_along_axis(query_position_rows, c2p_index, axis=2)
        key_pos = jnp.einsum('jhd,bhd->hjb', key_s, pos_query, precision=exact_precision_option)
        from_pos = jnp.swapaxes(jnp.take_along_axis(key_pos, c2p_index, axis=2), 1, 2)
        raw_sum = low_back(content + to_pos + from_pos)
        same_doc = seg_s[:, None] == seg_s[None, :]
        scores = jnp.where(same_doc[None], raw_sum * score_scale, neg_fill)
        weights_p = low(jax.nn.softmax(scores, axis=-1))
        context = jnp.einsum('hij,jhd->ihd', weights_p, value_s, precision=exact_precision_option)
        return (running, low(low_back(context)).reshape(length, H * HD))
    _, contexts = lax.scan(jax.checkpoint(attend), jnp.zeros((), jnp.float32), (queries, keys_all, values_all, segments))
    flattened_context = contexts.reshape(-1, model_width)
    branch = low_back(project(flattened_context, w_output))
    normed = layer_norm(flat_rows + branch, gain_attn, bias_attn)
    hidden = low_back(project(low(normed), w_up))
    activated = low(jax.nn.gelu(hidden, approximate=False))
    ffn_out = low_back(project(activated, w_down))
    result = layer_norm(normed + ffn_out, gain_ffn, bias_ffn)
    return result.reshape(count_seq, length, model_width)

def reference(inputs, cotangent, segments, buckets, w_query, w_key, w_value, w_output, w_up, w_down, positions, gain_attn, bias_attn, gain_ffn, bias_ffn):
    floats = [arg.astype(jnp.float32) for arg in (inputs, w_query, w_key, w_value, w_output, w_up, w_down, positions, gain_attn, bias_attn, gain_ffn, bias_ffn)]

    def wrapped(*params):
        return forward(*params, segments, buckets)
    result, pullback = jax.vjp(wrapped, *floats)
    gradients = pullback(cotangent.astype(jnp.float32))
    return (result.astype(jnp.bfloat16), gradients[0].astype(jnp.bfloat16), gradients[1], gradients[2], gradients[3], gradients[4], gradients[5], gradients[6], gradients[7], gradients[8], gradients[9], gradients[10], gradients[11])
```

```python
import functools
import math
from functools import partial
import jax, jax.numpy as jnp
from jax import lax
from jax.experimental import pallas as pl
from jax.experimental.pallas import tpu as pltpu
HD=64
NEG=-1000000000.0
TILE=128
F32=jnp.float32
BF=jnp.bfloat16

def dotf(a,b,ca,cb,precision=None):
    return lax.dot_general(a,b,(((ca,),(cb,)),((),())),preferred_element_type=F32,precision=precision)

def reversal(n,dtype):
    r=lax.broadcasted_iota(jnp.int32,(n,n),0); c=lax.broadcasted_iota(jnp.int32,(n,n),1)
    return (r+c==n-1).astype(F32).astype(dtype)

def attend_kernel(q_ref,k_ref,v_ref,kd_ref,pq_ref,sq_ref,sk_ref,ctx_ref,p_ref,st_ref,*,scale):
    rows=q_ref.shape[1]; total=k_ref.shape[1]; tile=min(TILE,rows)
    same_row=sk_ref[0]
    for half in range(2):
        cols=slice(half*HD,(half+1)*HD)
        q=q_ref[0][:,cols]; k=k_ref[0][:,cols]; v=v_ref[0][:,cols]
        kd=kd_ref[:,cols]; pq=pq_ref[:,cols]
        for j0 in range(0,total,TILE):
            width=rows+TILE; start=total-j0-TILE
            b=dotf(k[j0:j0+TILE],pq[start:start+width],1,1)
            b=pltpu.roll(b,width-TILE+1,axis=1,stride=1,stride_axis=0)[:,:rows]
            st_ref[:,j0:j0+TILE]=b.T
        for i0 in range(0,rows,tile):
            width=total+tile; start=rows-i0-tile
            qt=q[i0:i0+tile]
            a=dotf(qt,kd[start:start+width],1,1)
            a=pltpu.roll(a,width-tile+1,axis=1,stride=1,stride_axis=0)[:,:total]
            raw=dotf(qt,k,1,1)+a+st_ref[i0:i0+tile,:]
            s=jnp.where(sq_ref[0][i0:i0+tile]==same_row,raw*scale,NEG)
            e=jnp.exp(s-jnp.max(s,axis=1,keepdims=True))
            p=e*(1.0/jnp.sum(e,axis=1,keepdims=True))
            p_ref[0,half,i0:i0+tile,:]=p
            ctx_ref[0,i0:i0+tile,cols]=dotf(p.astype(BF),v,1,0).astype(BF)

def attend_back_kernel(q_ref,k_ref,v_ref,kd_ref,pq_ref,p_ref,dc_ref,dq_ref,dk_ref,dv_ref,dkd_ref,dpq_ref,ds_ref,pl_ref,dkt_ref,*,scale):
    rows=q_ref.shape[1]; total=k_ref.shape[1]; tile=min(TILE,rows)
    @pl.when(pl.program_id(1)==0)
    def _():
        dkd_ref[...]=jnp.zeros_like(dkd_ref)
        dpq_ref[...]=jnp.zeros_like(dpq_ref)
    flip_t=reversal(tile,BF); flip_j=reversal(TILE,BF)
    hi=lax.Precision.HIGHEST
    for half in range(2):
        cols=slice(half*HD,(half+1)*HD)
        q=q_ref[0][:,cols]; k=k_ref[0][:,cols]; v=v_ref[0][:,cols]; dc=dc_ref[0][:,cols]
        kd=kd_ref[:,cols]; pq=pq_ref[:,cols]
        for i0 in range(0,rows,tile):
            width=total+tile; start=rows-i0-tile
            p=p_ref[0,half,i0:i0+tile,:]
            dp=dotf(dc[i0:i0+tile],v,1,1)
            inner=jnp.sum(p*dp,axis=1,keepdims=True)
            ds=(p*(dp-inner)*scale).astype(BF)
            ds_ref[i0:i0+tile,:]=ds
            pl_ref[i0:i0+tile,:]=p.astype(BF)
            rev=dotf(flip_t,ds,1,0).astype(BF)
            rev=jnp.concatenate([rev,jnp.zeros((tile,tile),BF)],axis=1)
            rev=pltpu.roll(rev,0,axis=1,stride=1,stride_axis=0)
            qrev=dotf(flip_t,q[i0:i0+tile],1,0).astype(BF)
            dqr=dotf(rev,kd[start:start+width],1,0)
            dq=dotf(ds,k,1,0)+dotf(flip_t.astype(F32),dqr,1,0,hi)
            dq_ref[0,i0:i0+tile,cols]=dq.astype(BF)
            dkd_ref[start:start+width,cols]+=dotf(rev,qrev,0,0)
        dsf=ds_ref[...]
        dv_ref[0,:,cols]=dotf(pl_ref[...],dc,0,0).astype(BF)
        dkt_ref[...]=dotf(dsf,q,0,0)
        for j0 in range(0,total,TILE):
            width=rows+TILE; start=total-j0-TILE
            rev=dotf(flip_j,ds_ref[:,j0:j0+TILE],1,1).astype(BF)
            rev=jnp.concatenate([rev,jnp.zeros((TILE,TILE),BF)],axis=1)
            rev=pltpu.roll(rev,0,axis=1,stride=1,stride_axis=0)
            krev=dotf(flip_j,k[j0:j0+TILE],1,0).astype(BF)
            dkr=dotf(rev,pq[start:start+width],1,0)
            dk=dkt_ref[j0:j0+TILE,:]+dotf(flip_j.astype(F32),dkr,1,0,hi)
            dk_ref[0,j0:j0+TILE,cols]=dk.astype(BF)
            dpq_ref[start:start+width,cols]+=dotf(rev,krev,0,0)

def attend(q,k,v,kd,pq,sq,sk,scale):
    S,L,Wd=q.shape; T=k.shape[1]; W=kd.shape[0]; pairs=Wd//128
    row=lambda n:pl.BlockSpec((1,n,128),lambda s,h:(s,0,h))
    tab=pl.BlockSpec((W,128),lambda s,h:(0,h))
    return pl.pallas_call(functools.partial(attend_kernel,scale=scale),grid=(S,pairs),
      in_specs=[row(L),row(T),row(T),tab,tab,pl.BlockSpec((1,L,1),lambda s,h:(s,0,0)),pl.BlockSpec((1,1,T),lambda s,h:(s,0,0))],
      out_specs=[row(L),pl.BlockSpec((1,2,L,T),lambda s,h:(s,h,0,0))],
      out_shape=[jax.ShapeDtypeStruct((S,L,Wd),BF),jax.ShapeDtypeStruct((S,Wd//HD,L,T),F32)],
      scratch_shapes=[pltpu.VMEM((L,T),F32)],name="attend",
      cost_estimate=pl.CostEstimate(flops=int(16*S*L*T*Wd),bytes_accessed=int(S*L*T*Wd//HD*4),transcendentals=S*L*T*Wd//HD))(q,k,v,kd,pq,sq,sk)

def attend_back(q,k,v,kd,pq,p,dc,scale):
    S,L,Wd=q.shape; T=k.shape[1]; W=kd.shape[0]; pairs=Wd//128
    row=lambda n:pl.BlockSpec((1,n,128),lambda h,s:(s,0,h))
    tab=pl.BlockSpec((W,128),lambda h,s:(0,h))
    return pl.pallas_call(functools.partial(attend_back_kernel,scale=scale),grid=(pairs,S),
      in_specs=[row(L),row(T),row(T),tab,tab,pl.BlockSpec((1,2,L,T),lambda h,s:(s,h,0,0)),row(L)],
      out_specs=[row(L),row(T),row(T),tab,tab],
      out_shape=[jax.ShapeDtypeStruct((S,n,Wd),BF) for n in (L,T,T)]+[jax.ShapeDtypeStruct((W,Wd),F32)]*2,
      scratch_shapes=[pltpu.VMEM((L,T),BF),pltpu.VMEM((L,T),BF),pltpu.VMEM((T,HD),F32)],name="attend_back",
      cost_estimate=pl.CostEstimate(flops=int(32*S*L*T*Wd),bytes_accessed=int(S*L*T*Wd//HD*4),transcendentals=0))(q,k,v,kd,pq,p,dc)


BOTH = ("shard", "context")
eps_norm = 1e-06


def layer_norm(values, gain_row, shift_row):
    center = values - jnp.mean(values, axis=-1, keepdims=True)
    spread = jnp.mean(center * center, axis=-1, keepdims=True)
    return center * lax.rsqrt(spread + eps_norm) * gain_row + shift_row


def gelu_exact(values):
    return jax.nn.gelu(values, approximate=False)


def split_columns(packed, widths):
    at, out = 0, []
    for width in widths:
        out.append(packed[:, at:at + width])
        at += width
    return out


def local(inputs, cotangent, segments, buckets, w_query, w_key, w_value, w_output, w_up, w_down,
          positions, gain_attn, bias_attn, gain_ffn, bias_ffn):
    S, L, D = inputs.shape
    T = segments.shape[1]
    Wd = w_query.shape[1]
    F = w_up.shape[1]
    B = positions.shape[0]
    scale = 1.0 / math.sqrt(3 * HD)
    first = lax.axis_index("context") * L
    W = T + L
    own = w_query.shape[0]
    norms = jnp.stack([gain_attn, bias_attn, gain_ffn, bias_ffn], axis=1)
    norms = jnp.pad(norms, ((0, 0), (0, 124)))
    pack = jnp.concatenate([w_query, w_key, w_value, w_output.T, positions.T, norms], axis=1)
    pack = lax.all_gather(pack, BOTH, axis=0, tiled=True)
    wq, wk, wv, wo_t, pos_t, norms = split_columns(pack, (Wd, Wd, Wd, Wd, B, 128))
    pack = lax.all_gather(jnp.concatenate([w_up, w_down.T], axis=1), BOTH, axis=0, tiled=True)
    up, down_t = split_columns(pack, (F, F))
    gain_one, shift_one, gain_two, shift_two = [norms[:, i].astype(F32) for i in range(4)]
    rows = inputs.reshape(S * L, D)
    qkv = dotf(rows, jnp.concatenate([wq, wk, wv], axis=1), 1, 0).astype(BF)
    q, k, v = [x.reshape(S, L, Wd) for x in split_columns(qkv, (Wd, Wd, Wd))]
    k, v = split_last(lax.all_gather(jnp.concatenate([k, v], axis=2), "context", axis=1, tiled=True), Wd)
    pos_qk = dotf(pos_t, jnp.concatenate([wq, wk], axis=1), 0, 0).astype(BF)
    flipped = jnp.concatenate([buckets[::-1], buckets[:1]])
    to = lax.dynamic_slice_in_dim(flipped, T - L - first, W, 0)
    fro = lax.dynamic_slice_in_dim(flipped, first, W, 0)
    ids = jnp.arange(B, dtype=jnp.int32)
    pick_to = (to[:, None] == ids[None]).astype(BF)
    pick_from = (fro[:, None] == ids[None]).astype(BF)
    kd = dotf(pick_to, pos_qk[:, Wd:], 1, 0).astype(BF)
    pq = dotf(pick_from, pos_qk[:, :Wd], 1, 0).astype(BF)
    seg_here = lax.dynamic_slice_in_dim(segments, first, L, 1)[:, :, None]
    ctx, probs = attend(q, k, v, kd, pq, seg_here, segments[:, None, :], scale)
    ctx_rows = ctx.reshape(S * L, Wd)
    branch = lax.psum(dotf(ctx_rows, wo_t, 1, 1).astype(BF), "tensor").astype(F32)
    normed, pull_one = jax.vjp(layer_norm, rows.astype(F32) + branch, gain_one, shift_one)
    normed_low = normed.astype(BF)
    hidden = dotf(normed_low, up, 1, 0)
    act, pull_gelu = jax.vjp(gelu_exact, hidden)
    act_low = act.astype(BF)
    ffn = lax.psum(dotf(act_low, down_t, 1, 1).astype(BF), "tensor").astype(F32)
    result, pull_two = jax.vjp(layer_norm, normed + ffn, gain_two, shift_two)
    outputs = result.astype(BF).reshape(inputs.shape)
    d_second, d_gain_two, d_shift_two = pull_two(cotangent.reshape(S * L, D).astype(F32))
    d_ffn = d_second.astype(BF)
    d_act = dotf(d_ffn, down_t, 1, 0)
    g_down_t = dotf(d_ffn, act_low, 0, 0)
    d_hidden = pull_gelu(d_act)[0].astype(BF)
    g_up = dotf(normed_low, d_hidden, 0, 0)
    scatter = partial(lax.psum_scatter, axis_name=BOTH, scatter_dimension=0, tiled=True)
    g_ffn = scatter(jnp.concatenate([g_up.astype(BF), g_down_t.astype(BF)], axis=1))
    d_normed = d_second + lax.psum(dotf(d_hidden, up, 1, 1).astype(BF), "tensor").astype(F32)
    d_first, d_gain_one, d_shift_one = pull_one(d_normed)
    d_branch = d_first.astype(BF)
    d_ctx = dotf(d_branch, wo_t, 1, 0).astype(BF)
    g_out_t = dotf(d_branch, ctx_rows, 0, 0)
    dq, dk, dv, dkd, dpq = attend_back(q, k, v, kd, pq, probs, d_ctx.reshape(S, L, Wd), scale)
    dkv = lax.psum_scatter(jnp.concatenate([dk, dv], axis=2), "context", scatter_dimension=1, tiled=True)
    dqkv = jnp.concatenate([dq, dkv], axis=2).reshape(S * L, 3 * Wd)
    weights = jnp.concatenate([wq, wk, wv], axis=1)
    d_in = lax.psum(dotf(dqkv, weights, 1, 1).astype(BF), "tensor").astype(F32)
    grad_inputs = (d_first + d_in).astype(BF).reshape(inputs.shape)
    d_pos_key = dotf(pick_to, dkd.astype(BF), 0, 0)
    d_pos_query = dotf(pick_from, dpq.astype(BF), 0, 0)
    d_pos = jnp.concatenate([d_pos_query, d_pos_key], axis=1).astype(BF)
    g_qkv = dotf(rows, dqkv, 0, 0)
    g_pos_t = dotf(jnp.concatenate([wq, wk], axis=1), d_pos, 1, 1)
    g_qk = g_qkv[:, :2 * Wd] + dotf(pos_t, d_pos, 1, 0)
    g_norm = jnp.pad(jnp.stack([d_gain_one, d_shift_one, d_gain_two, d_shift_two], axis=1), ((0, 0), (0, 124)))
    pack = jnp.concatenate([x.astype(BF) for x in (g_qk, g_qkv[:, 2 * Wd:], g_out_t, g_pos_t, g_norm)], axis=1)
    g_q, g_k, g_v, g_o, g_p, g_n = split_columns(scatter(pack), (Wd, Wd, Wd, Wd, B, 128))
    g_p = lax.psum(g_p, "tensor")
    f = lambda x: x.astype(F32)
    return (outputs, grad_inputs, f(g_q), f(g_k), f(g_v), f(g_o).T, f(g_ffn[:, :F]), f(g_ffn[:, F:]).T, f(g_p).T,
            f(g_n[:, 0]), f(g_n[:, 1]), f(g_n[:, 2]), f(g_n[:, 3]))


def split_last(packed, width):
    return packed[..., :width], packed[..., width:]


def solution(mesh):
    P = jax.sharding.PartitionSpec
    act, row, col, vec = P("shard", "context", None), P(BOTH, "tensor"), P("tensor", BOTH), P(BOTH)
    return jax.shard_map(local, mesh=mesh,
        in_specs=(act, act, P("shard", None), P(), row, row, row, col, row, col, P(None, BOTH), vec, vec, vec, vec),
        out_specs=(act, act, row, row, row, col, row, col, P(None, BOTH), vec, vec, vec, vec),
        check_vma=False)
```

```python
import functools
import math
from functools import partial
import jax, jax.numpy as jnp
from jax import lax
from jax.experimental import pallas as pl
from jax.experimental.pallas import tpu as pltpu
HD=64
NEG=-1000000000.0
TILE=128
F32=jnp.float32
BF=jnp.bfloat16

def dotf(a,b,ca,cb,precision=None):
    return lax.dot_general(a,b,(((ca,),(cb,)),((),())),preferred_element_type=F32,precision=precision)

def reversal(n,dtype):
    r=lax.broadcasted_iota(jnp.int32,(n,n),0); c=lax.broadcasted_iota(jnp.int32,(n,n),1)
    return (r+c==n-1).astype(F32).astype(dtype)

def attend_kernel(q_ref,k_ref,v_ref,kd_ref,pq_ref,sq_ref,sk_ref,ctx_ref,p_ref,st_ref,*,scale):
    rows=q_ref.shape[1]; total=k_ref.shape[1]; tile=min(TILE,rows)
    same_row=sk_ref[0]
    for half in range(2):
        cols=slice(half*HD,(half+1)*HD)
        q=q_ref[0][:,cols]; k=k_ref[0][:,cols]; v=v_ref[0][:,cols]
        kd=kd_ref[:,cols]; pq=pq_ref[:,cols]
        for j0 in range(0,total,TILE):
            width=rows+TILE; start=total-j0-TILE
            b=dotf(k[j0:j0+TILE],pq[start:start+width],1,1)
            b=pltpu.roll(b,width-TILE+1,axis=1,stride=1,stride_axis=0)[:,:rows]
            st_ref[:,j0:j0+TILE]=b.T
        for i0 in range(0,rows,tile):
            width=total+tile; start=rows-i0-tile
            qt=q[i0:i0+tile]
            a=dotf(qt,kd[start:start+width],1,1)
            a=pltpu.roll(a,width-tile+1,axis=1,stride=1,stride_axis=0)[:,:total]
            raw=dotf(qt,k,1,1)+a+st_ref[i0:i0+tile,:]
            s=jnp.where(sq_ref[0][i0:i0+tile]==same_row,raw*scale,NEG)
            e=jnp.exp(s-jnp.max(s,axis=1,keepdims=True))
            p=e*(1.0/jnp.sum(e,axis=1,keepdims=True))
            p_ref[0,half,i0:i0+tile,:]=p
            ctx_ref[0,i0:i0+tile,cols]=dotf(p.astype(BF),v,1,0).astype(BF)

def attend_back_kernel(q_ref,k_ref,v_ref,kd_ref,pq_ref,p_ref,dc_ref,dq_ref,dk_ref,dv_ref,dkd_ref,dpq_ref,ds_ref,pl_ref,dkt_ref,*,scale):
    rows=q_ref.shape[1]; total=k_ref.shape[1]; tile=min(TILE,rows)
    @pl.when(pl.program_id(1)==0)
    def _():
        dkd_ref[...]=jnp.zeros_like(dkd_ref)
        dpq_ref[...]=jnp.zeros_like(dpq_ref)
    flip_t=reversal(tile,BF); flip_j=reversal(TILE,BF)
    hi=lax.Precision.HIGHEST
    for half in range(2):
        cols=slice(half*HD,(half+1)*HD)
        q=q_ref[0][:,cols]; k=k_ref[0][:,cols]; v=v_ref[0][:,cols]; dc=dc_ref[0][:,cols]
        kd=kd_ref[:,cols]; pq=pq_ref[:,cols]
        for i0 in range(0,rows,tile):
            width=total+tile; start=rows-i0-tile
            p=p_ref[0,half,i0:i0+tile,:]
            dp=dotf(dc[i0:i0+tile],v,1,1)
            inner=jnp.sum(p*dp,axis=1,keepdims=True)
            ds=(p*(dp-inner)*scale).astype(BF)
            ds_ref[i0:i0+tile,:]=ds
            pl_ref[i0:i0+tile,:]=p.astype(BF)
            rev=dotf(flip_t,ds,1,0).astype(BF)
            rev=jnp.concatenate([rev,jnp.zeros((tile,tile),BF)],axis=1)
            rev=pltpu.roll(rev,0,axis=1,stride=1,stride_axis=0)
            qrev=dotf(flip_t,q[i0:i0+tile],1,0).astype(BF)
            dqr=dotf(rev,kd[start:start+width],1,0)
            dq=dotf(ds,k,1,0)+dotf(flip_t.astype(F32),dqr,1,0,hi)
            dq_ref[0,i0:i0+tile,cols]=dq.astype(BF)
            dkd_ref[start:start+width,cols]+=dotf(rev,qrev,0,0)
        dsf=ds_ref[...]
        dv_ref[0,:,cols]=dotf(pl_ref[...],dc,0,0).astype(BF)
        dkt_ref[...]=dotf(dsf,q,0,0)
        for j0 in range(0,total,TILE):
            width=rows+TILE; start=total-j0-TILE
            rev=dotf(flip_j,ds_ref[:,j0:j0+TILE],1,1).astype(BF)
            rev=jnp.concatenate([rev,jnp.zeros((TILE,TILE),BF)],axis=1)
            rev=pltpu.roll(rev,0,axis=1,stride=1,stride_axis=0)
            krev=dotf(flip_j,k[j0:j0+TILE],1,0).astype(BF)
            dkr=dotf(rev,pq[start:start+width],1,0)
            dk=dkt_ref[j0:j0+TILE,:]+dotf(flip_j.astype(F32),dkr,1,0,hi)
            dk_ref[0,j0:j0+TILE,cols]=dk.astype(BF)
            dpq_ref[start:start+width,cols]+=dotf(rev,krev,0,0)

def attend(q,k,v,kd,pq,sq,sk,scale):
    S,L,Wd=q.shape; T=k.shape[1]; W=kd.shape[0]; pairs=Wd//128
    row=lambda n:pl.BlockSpec((1,n,128),lambda s,h:(s,0,h))
    tab=pl.BlockSpec((W,128),lambda s,h:(0,h))
    return pl.pallas_call(functools.partial(attend_kernel,scale=scale),grid=(S,pairs),
      in_specs=[row(L),row(T),row(T),tab,tab,pl.BlockSpec((1,L,1),lambda s,h:(s,0,0)),pl.BlockSpec((1,1,T),lambda s,h:(s,0,0))],
      out_specs=[row(L),pl.BlockSpec((1,2,L,T),lambda s,h:(s,h,0,0))],
      out_shape=[jax.ShapeDtypeStruct((S,L,Wd),BF),jax.ShapeDtypeStruct((S,Wd//HD,L,T),F32)],
      scratch_shapes=[pltpu.VMEM((L,T),F32)],name="attend",
      cost_estimate=pl.CostEstimate(flops=int(16*S*L*T*Wd),bytes_accessed=int(S*L*T*Wd//HD*4),transcendentals=S*L*T*Wd//HD))(q,k,v,kd,pq,sq,sk)

def attend_back(q,k,v,kd,pq,p,dc,scale):
    S,L,Wd=q.shape; T=k.shape[1]; W=kd.shape[0]; pairs=Wd//128
    row=lambda n:pl.BlockSpec((1,n,128),lambda h,s:(s,0,h))
    tab=pl.BlockSpec((W,128),lambda h,s:(0,h))
    return pl.pallas_call(functools.partial(attend_back_kernel,scale=scale),grid=(pairs,S),
      in_specs=[row(L),row(T),row(T),tab,tab,pl.BlockSpec((1,2,L,T),lambda h,s:(s,h,0,0)),row(L)],
      out_specs=[row(L),row(T),row(T),tab,tab],
      out_shape=[jax.ShapeDtypeStruct((S,n,Wd),BF) for n in (L,T,T)]+[jax.ShapeDtypeStruct((W,Wd),F32)]*2,
      scratch_shapes=[pltpu.VMEM((L,T),BF),pltpu.VMEM((L,T),BF),pltpu.VMEM((T,HD),F32)],name="attend_back",
      cost_estimate=pl.CostEstimate(flops=int(32*S*L*T*Wd),bytes_accessed=int(S*L*T*Wd//HD*4),transcendentals=0))(q,k,v,kd,pq,p,dc)


BOTH = ("shard", "context")
eps_norm = 1e-06

MESH = pl.DeviceIdType.MESH
ROUNDS = 8


class Line:
    def __init__(self, n, chunk, send, from_left, from_right, total, sems):
        self.n, self.chunk, self.owner = n, chunk, n // 2 - 1
        self.send, self.from_left, self.from_right, self.total, self.sems = send, from_left, from_right, total, sems

    def at(self, half, k):
        p = lax.axis_index("tensor")
        rows = pl.ds(pl.multiple_of((2 * k + half) * self.chunk, self.chunk), self.chunk)
        q = p if half == 0 else self.n - 1 - p
        return q, p + 1 - 2 * half, p - 1 + 2 * half, rows

    def copy(self, half, k, kind, source, target, recv, device, rows):
        return pltpu.make_async_remote_copy(
            src_ref=source.at[rows, :], dst_ref=target.at[rows, :], send_sem=self.sems.at[kind, half, k],
            recv_sem=self.sems.at[recv, half, k], device_id={"tensor": device}, device_id_type=MESH)

    def inward_left(self, half, k):
        q, right, left, rows = self.at(half, k)
        return self.copy(half, k, 0, self.send, self.from_right, 2, left, rows)

    def inward_right(self, half, k):
        q, right, left, rows = self.at(half, k)
        return self.copy(half, k, 0, self.send, self.from_left, 1, right, rows)

    def outward_right(self, half, k):
        q, right, left, rows = self.at(half, k)
        return self.copy(half, k, 3, self.total, self.total, 5, right, rows)

    def outward_left(self, half, k):
        q, right, left, rows = self.at(half, k)
        return self.copy(half, k, 4, self.total, self.total, 5, left, rows)

    def edge(self, half, k):
        q = self.at(half, k)[0]

        @pl.when(q == self.n - 1)
        def _():
            self.inward_left(half, k).start()
        if self.owner > 0:
            @pl.when(q == 0)
            def _():
                self.inward_right(half, k).start()

    def mid(self, half, k):
        n, o = self.n, self.owner
        q, right, left, rows = self.at(half, k)
        if n - 1 - o > 1:
            @pl.when((q > o) & (q < n - 1))
            def _():
                self.inward_left(half, k).wait_recv()
                self.send[rows, :] = (self.send[rows, :].astype(F32) + self.from_right[rows, :].astype(F32)).astype(BF)
                self.inward_left(half, k).start()
        if o > 1:
            @pl.when((q < o) & (q > 0))
            def _():
                self.inward_right(half, k).wait_recv()
                self.send[rows, :] = (self.send[rows, :].astype(F32) + self.from_left[rows, :].astype(F32)).astype(BF)
                self.inward_right(half, k).start()

    def own(self, half, k):
        o = self.owner
        q, right, left, rows = self.at(half, k)

        @pl.when(q == o)
        def _():
            self.inward_left(half, k).wait_recv()
            total = self.send[rows, :].astype(F32) + self.from_right[rows, :].astype(F32)
            if o > 0:
                self.inward_right(half, k).wait_recv()
                total = total + self.from_left[rows, :].astype(F32)
            self.total[rows, :] = total.astype(BF)
            self.outward_right(half, k).start()
            if o > 0:
                self.outward_left(half, k).start()

    def forward(self, half, k):
        n, o = self.n, self.owner
        q = self.at(half, k)[0]

        @pl.when(q > o)
        def _():
            self.outward_right(half, k).wait_recv()

            @pl.when(q < n - 1)
            def _():
                self.outward_right(half, k).start()
        if o > 0:
            @pl.when(q < o)
            def _():
                self.outward_left(half, k).wait_recv()

                @pl.when(q > 0)
                def _():
                    self.outward_left(half, k).start()

    def drain(self, half, k):
        n, o = self.n, self.owner
        q = self.at(half, k)[0]

        @pl.when(q != o)
        def _():
            self.inward_left(half, k).wait_send()

        @pl.when((q >= o) & (q < n - 1))
        def _():
            self.outward_right(half, k).wait_send()
        if o > 0:
            @pl.when((q <= o) & (q > 0))
            def _():
                self.outward_left(half, k).wait_send()


def greet_line(n):
    p = lax.axis_index("tensor")
    barrier = pltpu.get_barrier_semaphore()

    @pl.when(p > 0)
    def _():
        pl.semaphore_signal(barrier, inc=1, device_id={"tensor": p - 1}, device_id_type=MESH)

    @pl.when(p < n - 1)
    def _():
        pl.semaphore_signal(barrier, inc=1, device_id={"tensor": p + 1}, device_id_type=MESH)

    inner = (p > 0) & (p < n - 1)

    @pl.when(inner)
    def _():
        pl.semaphore_wait(barrier, 2)

    @pl.when(jnp.logical_not(inner))
    def _():
        pl.semaphore_wait(barrier, 1)


def standardize(values):
    center = values - jnp.mean(values, axis=1, keepdims=True)
    rate = lax.rsqrt(jnp.mean(center * center, axis=1, keepdims=True) + eps_norm)
    return center * rate, rate


def norm_back(grad, unit, rate, gain):
    scaled = grad * gain
    return rate * (scaled - jnp.mean(scaled, axis=1, keepdims=True) - unit * jnp.mean(scaled * unit, axis=1, keepdims=True))


def middle_kernel(n, ctx, rows, wo_t, norms, cot_hbm, up_hbm, down_hbm, outputs, d_first, d_ctx, g_up, g_down, g_out, g_norm,
                  cot, up, down, low, act, d_ffn, d_hid, d_br, unit, slope, d_sec, rates, sums, load_sems, *line_refs):
    R, D = rows.shape
    chunk = R // (2 * ROUNDS)
    pair = 2 * chunk
    loads = [pltpu.make_async_copy(a, b, load_sems.at[i]) for i, (a, b) in
             enumerate([(up_hbm, up), (down_hbm, down), (cot_hbm, cot)])]
    for load in loads:
        load.start()
    lines = [Line(n, chunk, *line_refs[5 * i:5 * i + 5]) for i in range(3)]
    greet_line(n)
    sums[...] = jnp.zeros_like(sums)

    def add_sum(i, values):
        sums[8 * i:8 * i + 8, :] += jnp.sum(values.reshape(pair // 8, 8, D), axis=0)

    def pair_rows(k):
        return pl.ds(pl.multiple_of(k * pair, pair), pair)

    def open_first(k):
        r = pair_rows(k)
        lines[0].send[r, :] = dotf(ctx[r, :], wo_t[...], 1, 1).astype(BF)

    def first_to_second(k):
        r = pair_rows(k)
        u, rate = standardize(rows[r, :].astype(F32) + lines[0].total[r, :].astype(F32))
        unit[r, :] = u
        rates[r, :] = jnp.broadcast_to(rate, (pair, 128))
        nl = (u * norms[0:1, :] + norms[1:2, :]).astype(BF)
        low[r, :] = nl
        hidden = dotf(nl, up[...], 1, 0)
        half_cdf = 0.5 * (1.0 + lax.erf(hidden * 0.7071067811865476))
        slope[r, :] = half_cdf + hidden * (jnp.exp(-0.5 * hidden * hidden) * 0.3989422804014327)
        a = (hidden * half_cdf).astype(BF)
        act[r, :] = a
        lines[1].send[r, :] = dotf(a, down[...], 1, 1).astype(BF)

    def second_to_third(k):
        r = pair_rows(k)
        u, rate = standardize(unit[r, :] * norms[0:1, :] + norms[1:2, :] + lines[1].total[r, :].astype(F32))
        outputs[r, :] = (u * norms[2:3, :] + norms[3:4, :]).astype(BF)
        g = cot[r, :].astype(F32)
        add_sum(2, g * u)
        add_sum(3, g)
        ds = norm_back(g, u, rate, norms[2:3, :])
        d_sec[r, :] = ds
        dl = ds.astype(BF)
        d_ffn[r, :] = dl
        dh = (dotf(dl, down[...], 1, 0) * slope[r, :]).astype(BF)
        d_hid[r, :] = dh
        lines[2].send[r, :] = dotf(dh, up[...], 1, 1).astype(BF)

    def close_third(k):
        r = pair_rows(k)
        g = d_sec[r, :] + lines[2].total[r, :].astype(F32)
        u = unit[r, :]
        add_sum(0, g * u)
        add_sum(1, g)
        d1 = norm_back(g, u, rates[r, 0:1], norms[0:1, :])
        d_first[r, :] = d1
        db = d1.astype(BF)
        d_br[r, :] = db
        d_ctx[r, :] = dotf(db, wo_t[...], 1, 0).astype(BF)

    def weight_grad(out, left, right):
        width = min(256, D)

        def tile(i, _):
            c = pl.ds(pl.multiple_of(i * width, width), width)
            out[c, :] = dotf(left[:, c], right[...], 0, 0).astype(BF)
            return 0
        lax.fori_loop(0, D // width, tile, 0)

    def when_valid(t, lag, body):
        @pl.when((t >= lag) & (t < lag + ROUNDS))
        def _():
            body(t - lag)

    def both(stage):
        def run(k):
            stage(0, k)
            stage(1, k)
        return run

    def start(line, body):
        def run(k):
            body(k)
            line.edge(0, k)
            line.edge(1, k)
        return run

    def step(t, _):
        for i in (2, 1, 0):
            for lag, stage in ((8, lines[i].forward), (6, lines[i].own), (4, lines[i].mid)):
                when_valid(t, 8 * i + lag, both(stage))
        when_valid(t, 24, close_third)
        when_valid(t, 16, start(lines[2], second_to_third))
        when_valid(t, 8, start(lines[1], first_to_second))
        when_valid(t, 0, start(lines[0], open_first))

        @pl.when(t == 7)
        def _():
            for load in loads:
                load.wait()

        @pl.when(t == 16 + ROUNDS)
        def _():
            weight_grad(g_down, d_ffn, act)

        @pl.when(t == 17 + ROUNDS)
        def _():
            weight_grad(g_up, low, d_hid)
        return 0

    lax.fori_loop(0, ROUNDS + 24, step, 0)
    weight_grad(g_out, d_br, ctx)
    for i in range(4):
        g_norm[i:i + 1, :] = jnp.sum(sums[8 * i:8 * i + 8, :], axis=0, keepdims=True)
    g_norm[4:8, :] = jnp.zeros((4, D), F32)

    def finish(k, _):
        for line in lines:
            line.drain(0, k)
            line.drain(1, k)
        return 0
    lax.fori_loop(0, ROUNDS, finish, 0)


def middle(n, ctx, rows, wo_t, norms, cot, up, down):
    R, D = rows.shape
    Wd, F = wo_t.shape[1], up.shape[1]
    vmem, hbm = pl.BlockSpec(memory_space=pltpu.VMEM), pl.BlockSpec(memory_space=pl.ANY)
    line = [pltpu.VMEM((R, D), BF)] * 4 + [pltpu.SemaphoreType.DMA((6, 2, ROUNDS))]
    shape = jax.ShapeDtypeStruct
    return pl.pallas_call(
        partial(middle_kernel, n),
        in_specs=[vmem] * 4 + [hbm] * 3,
        out_specs=[vmem] * 7,
        out_shape=[shape((R, D), BF), shape((R, D), F32), shape((R, Wd), BF), shape((D, F), BF), shape((D, F), BF),
                   shape((D, Wd), BF), shape((8, D), F32)],
        scratch_shapes=[pltpu.VMEM((R, D), BF), pltpu.VMEM((D, F), BF), pltpu.VMEM((D, F), BF), pltpu.VMEM((R, D), BF),
                        pltpu.VMEM((R, F), BF), pltpu.VMEM((R, D), BF), pltpu.VMEM((R, F), BF), pltpu.VMEM((R, D), BF),
                        pltpu.VMEM((R, D), F32), pltpu.VMEM((R, F), F32), pltpu.VMEM((R, D), F32), pltpu.VMEM((R, 128), F32),
                        pltpu.VMEM((32, D), F32), pltpu.SemaphoreType.DMA((3,))] + line * 3,
        compiler_params=pltpu.CompilerParams(collective_id=1, has_side_effects=True),
        name="middle",
        cost_estimate=pl.CostEstimate(flops=12 * R * D * F, bytes_accessed=16 * R * D, transcendentals=2 * R * F),
    )(ctx, rows, wo_t, norms, cot, up, down)


def split_columns(packed, widths):
    at, out = 0, []
    for width in widths:
        out.append(packed[:, at:at + width])
        at += width
    return out


def local(inputs, cotangent, segments, buckets, w_query, w_key, w_value, w_output, w_up, w_down,
          positions, gain_attn, bias_attn, gain_ffn, bias_ffn):
    S, L, D = inputs.shape
    T = segments.shape[1]
    Wd = w_query.shape[1]
    F = w_up.shape[1]
    B = positions.shape[0]
    scale = 1.0 / math.sqrt(3 * HD)
    first = lax.axis_index("context") * L
    W = T + L
    own = w_query.shape[0]
    norms = jnp.stack([gain_attn, bias_attn, gain_ffn, bias_ffn], axis=1)
    norms = jnp.pad(norms, ((0, 0), (0, 124)))
    pack = jnp.concatenate([w_query, w_key, w_value, w_output.T, positions.T, norms], axis=1)
    pack = lax.all_gather(pack, BOTH, axis=0, tiled=True)
    wq, wk, wv, wo_t, pos_t, norms = split_columns(pack, (Wd, Wd, Wd, Wd, B, 128))
    pack = lax.all_gather(jnp.concatenate([w_up, w_down.T], axis=1), BOTH, axis=0, tiled=True)
    up, down_t = split_columns(pack, (F, F))
    norms = jnp.pad(norms[:, :4].astype(F32).T, ((0, 4), (0, 0)))
    rows = inputs.reshape(S * L, D)
    qkv = dotf(rows, jnp.concatenate([wq, wk, wv], axis=1), 1, 0).astype(BF)
    q, k, v = [x.reshape(S, L, Wd) for x in split_columns(qkv, (Wd, Wd, Wd))]
    k, v = split_last(lax.all_gather(jnp.concatenate([k, v], axis=2), "context", axis=1, tiled=True), Wd)
    pos_qk = dotf(pos_t, jnp.concatenate([wq, wk], axis=1), 0, 0).astype(BF)
    flipped = jnp.concatenate([buckets[::-1], buckets[:1]])
    to = lax.dynamic_slice_in_dim(flipped, T - L - first, W, 0)
    fro = lax.dynamic_slice_in_dim(flipped, first, W, 0)
    ids = jnp.arange(B, dtype=jnp.int32)
    pick_to = (to[:, None] == ids[None]).astype(BF)
    pick_from = (fro[:, None] == ids[None]).astype(BF)
    kd = dotf(pick_to, pos_qk[:, Wd:], 1, 0).astype(BF)
    pq = dotf(pick_from, pos_qk[:, :Wd], 1, 0).astype(BF)
    seg_here = lax.dynamic_slice_in_dim(segments, first, L, 1)[:, :, None]
    ctx, probs = attend(q, k, v, kd, pq, seg_here, segments[:, None, :], scale)
    ctx_rows = ctx.reshape(S * L, Wd)
    outputs, d_first, d_ctx, g_up, g_down_t, g_out_t, g_norm = middle(
        lax.axis_size("tensor"), ctx_rows, rows, wo_t, norms, cotangent.reshape(S * L, D), up, down_t)
    outputs = outputs.reshape(inputs.shape)
    scatter = partial(lax.psum_scatter, axis_name=BOTH, scatter_dimension=0, tiled=True)
    g_ffn = scatter(jnp.concatenate([g_up, g_down_t], axis=1))
    dq, dk, dv, dkd, dpq = attend_back(q, k, v, kd, pq, probs, d_ctx.reshape(S, L, Wd), scale)
    dkv = lax.psum_scatter(jnp.concatenate([dk, dv], axis=2), "context", scatter_dimension=1, tiled=True)
    dqkv = jnp.concatenate([dq, dkv], axis=2).reshape(S * L, 3 * Wd)
    weights = jnp.concatenate([wq, wk, wv], axis=1)
    d_in = lax.psum(dotf(dqkv, weights, 1, 1).astype(BF), "tensor").astype(F32)
    grad_inputs = (d_first + d_in).astype(BF).reshape(inputs.shape)
    d_pos_key = dotf(pick_to, dkd.astype(BF), 0, 0)
    d_pos_query = dotf(pick_from, dpq.astype(BF), 0, 0)
    d_pos = jnp.concatenate([d_pos_query, d_pos_key], axis=1).astype(BF)
    g_qkv = dotf(rows, dqkv, 0, 0)
    g_pos_t = dotf(jnp.concatenate([wq, wk], axis=1), d_pos, 1, 1)
    g_qk = g_qkv[:, :2 * Wd] + dotf(pos_t, d_pos, 1, 0)
    g_norm = jnp.pad(g_norm.T, ((0, 0), (0, 120)))
    pack = jnp.concatenate([x.astype(BF) for x in (g_qk, g_qkv[:, 2 * Wd:], g_out_t, g_pos_t, g_norm)], axis=1)
    g_q, g_k, g_v, g_o, g_p, g_n = split_columns(scatter(pack), (Wd, Wd, Wd, Wd, B, 128))
    g_p = lax.psum(g_p, "tensor")
    f = lambda x: x.astype(F32)
    return (outputs, grad_inputs, f(g_q), f(g_k), f(g_v), f(g_o).T, f(g_ffn[:, :F]), f(g_ffn[:, F:]).T, f(g_p).T,
            f(g_n[:, 0]), f(g_n[:, 1]), f(g_n[:, 2]), f(g_n[:, 3]))


def split_last(packed, width):
    return packed[..., :width], packed[..., width:]


def solution(mesh):
    P = jax.sharding.PartitionSpec
    act, row, col, vec = P("shard", "context", None), P(BOTH, "tensor"), P("tensor", BOTH), P(BOTH)
    return jax.shard_map(local, mesh=mesh,
        in_specs=(act, act, P("shard", None), P(), row, row, row, col, row, col, P(None, BOTH), vec, vec, vec, vec),
        out_specs=(act, act, row, row, row, col, row, col, P(None, BOTH), vec, vec, vec, vec),
        check_vma=False)
```

```python
import functools
import math
from functools import partial
import jax, jax.numpy as jnp
from jax import lax
from jax.experimental import pallas as pl
from jax.experimental.pallas import tpu as pltpu
HD=64
NEG=-1000000000.0
TILE=128
F32=jnp.float32
BF=jnp.bfloat16

def dotf(a,b,ca,cb,precision=None):
    return lax.dot_general(a,b,(((ca,),(cb,)),((),())),preferred_element_type=F32,precision=precision)

def reversal(n,dtype):
    r=lax.broadcasted_iota(jnp.int32,(n,n),0); c=lax.broadcasted_iota(jnp.int32,(n,n),1)
    return (r+c==n-1).astype(F32).astype(dtype)

def attend_kernel(q_ref,k_ref,v_ref,kd_ref,pq_ref,sq_ref,sk_ref,ctx_ref,p_ref,st_ref,*,scale):
    rows=q_ref.shape[1]; total=k_ref.shape[1]; tile=min(TILE,rows)
    same_row=sk_ref[0]
    for half in range(2):
        cols=slice(half*HD,(half+1)*HD)
        q=q_ref[0][:,cols]; k=k_ref[0][:,cols]; v=v_ref[0][:,cols]
        kd=kd_ref[:,cols]; pq=pq_ref[:,cols]
        for j0 in range(0,total,TILE):
            width=rows+TILE; start=total-j0-TILE
            b=dotf(k[j0:j0+TILE],pq[start:start+width],1,1)
            b=pltpu.roll(b,width-TILE+1,axis=1,stride=1,stride_axis=0)[:,:rows]
            st_ref[:,j0:j0+TILE]=b.T
        for i0 in range(0,rows,tile):
            width=total+tile; start=rows-i0-tile
            qt=q[i0:i0+tile]
            a=dotf(qt,kd[start:start+width],1,1)
            a=pltpu.roll(a,width-tile+1,axis=1,stride=1,stride_axis=0)[:,:total]
            raw=dotf(qt,k,1,1)+a+st_ref[i0:i0+tile,:]
            s=jnp.where(sq_ref[0][i0:i0+tile]==same_row,raw*scale,NEG)
            e=jnp.exp(s-jnp.max(s,axis=1,keepdims=True))
            p=e*(1.0/jnp.sum(e,axis=1,keepdims=True))
            p_ref[0,half,i0:i0+tile,:]=p
            ctx_ref[0,i0:i0+tile,cols]=dotf(p.astype(BF),v,1,0).astype(BF)

def attend_back_kernel(q_ref,k_ref,v_ref,kd_ref,pq_ref,p_ref,dc_ref,dq_ref,dk_ref,dv_ref,dkd_ref,dpq_ref,ds_ref,pl_ref,dkt_ref,*,scale,between=None):
    rows=q_ref.shape[1]; total=k_ref.shape[1]; tile=min(TILE,rows)
    @pl.when(pl.program_id(1)==0)
    def _():
        dkd_ref[...]=jnp.zeros_like(dkd_ref)
        dpq_ref[...]=jnp.zeros_like(dpq_ref)
    flip_t=reversal(tile,BF); flip_j=reversal(TILE,BF)
    hi=lax.Precision.HIGHEST
    for half in range(2):
        cols=slice(half*HD,(half+1)*HD)
        q=q_ref[0][:,cols]; k=k_ref[0][:,cols]; v=v_ref[0][:,cols]; dc=dc_ref[0][:,cols]
        kd=kd_ref[:,cols]; pq=pq_ref[:,cols]
        for i0 in range(0,rows,tile):
            width=total+tile; start=rows-i0-tile
            p=p_ref[0,half,i0:i0+tile,:]
            dp=dotf(dc[i0:i0+tile],v,1,1)
            inner=jnp.sum(p*dp,axis=1,keepdims=True)
            ds=(p*(dp-inner)*scale).astype(BF)
            ds_ref[i0:i0+tile,:]=ds
            pl_ref[i0:i0+tile,:]=p.astype(BF)
            rev=dotf(flip_t,ds,1,0).astype(BF)
            rev=jnp.concatenate([rev,jnp.zeros((tile,tile),BF)],axis=1)
            rev=pltpu.roll(rev,0,axis=1,stride=1,stride_axis=0)
            qrev=dotf(flip_t,q[i0:i0+tile],1,0).astype(BF)
            dqr=dotf(rev,kd[start:start+width],1,0)
            dq=dotf(ds,k,1,0)+dotf(flip_t.astype(F32),dqr,1,0,hi)
            dq_ref[0,i0:i0+tile,cols]=dq.astype(BF)
            dkd_ref[start:start+width,cols]+=dotf(rev,qrev,0,0)
        dsf=ds_ref[...]
        dv_ref[0,:,cols]=dotf(pl_ref[...],dc,0,0).astype(BF)
        dkt_ref[...]=dotf(dsf,q,0,0)
        for j0 in range(0,total,TILE):
            width=rows+TILE; start=total-j0-TILE
            rev=dotf(flip_j,ds_ref[:,j0:j0+TILE],1,1).astype(BF)
            rev=jnp.concatenate([rev,jnp.zeros((TILE,TILE),BF)],axis=1)
            rev=pltpu.roll(rev,0,axis=1,stride=1,stride_axis=0)
            krev=dotf(flip_j,k[j0:j0+TILE],1,0).astype(BF)
            dkr=dotf(rev,pq[start:start+width],1,0)
            dk=dkt_ref[j0:j0+TILE,:]+dotf(flip_j.astype(F32),dkr,1,0,hi)
            dk_ref[0,j0:j0+TILE,cols]=dk.astype(BF)
            dpq_ref[start:start+width,cols]+=dotf(rev,krev,0,0)
        if between is not None:
            between(half)

def attend(q,k,v,kd,pq,sq,sk,scale):
    S,L,Wd=q.shape; T=k.shape[1]; W=kd.shape[0]; pairs=Wd//128
    row=lambda n:pl.BlockSpec((1,n,128),lambda s,h:(s,0,h))
    tab=pl.BlockSpec((W,128),lambda s,h:(0,h))
    return pl.pallas_call(functools.partial(attend_kernel,scale=scale),grid=(S,pairs),
      in_specs=[row(L),row(T),row(T),tab,tab,pl.BlockSpec((1,L,1),lambda s,h:(s,0,0)),pl.BlockSpec((1,1,T),lambda s,h:(s,0,0))],
      out_specs=[row(L),pl.BlockSpec((1,2,L,T),lambda s,h:(s,h,0,0))],
      out_shape=[jax.ShapeDtypeStruct((S,L,Wd),BF),jax.ShapeDtypeStruct((S,Wd//HD,L,T),F32)],
      scratch_shapes=[pltpu.VMEM((L,T),F32)],name="attend",
      cost_estimate=pl.CostEstimate(flops=int(16*S*L*T*Wd),bytes_accessed=int(S*L*T*Wd//HD*4),transcendentals=S*L*T*Wd//HD))(q,k,v,kd,pq,sq,sk)

def attend_back(q,k,v,kd,pq,p,dc,scale):
    S,L,Wd=q.shape; T=k.shape[1]; W=kd.shape[0]; pairs=Wd//128
    row=lambda n:pl.BlockSpec((1,n,128),lambda h,s:(s,0,h))
    tab=pl.BlockSpec((W,128),lambda h,s:(0,h))
    return pl.pallas_call(functools.partial(attend_back_kernel,scale=scale),grid=(pairs,S),
      in_specs=[row(L),row(T),row(T),tab,tab,pl.BlockSpec((1,2,L,T),lambda h,s:(s,h,0,0)),row(L)],
      out_specs=[row(L),row(T),row(T),tab,tab],
      out_shape=[jax.ShapeDtypeStruct((S,n,Wd),BF) for n in (L,T,T)]+[jax.ShapeDtypeStruct((W,Wd),F32)]*2,
      scratch_shapes=[pltpu.VMEM((L,T),BF),pltpu.VMEM((L,T),BF),pltpu.VMEM((T,HD),F32)],name="attend_back",
      cost_estimate=pl.CostEstimate(flops=int(32*S*L*T*Wd),bytes_accessed=int(S*L*T*Wd//HD*4),transcendentals=0))(q,k,v,kd,pq,p,dc)


BOTH = ("shard", "context")
eps_norm = 1e-06

MESH = pl.DeviceIdType.MESH
ROUNDS = 8


class Line:
    def __init__(self, n, chunk, send, from_left, from_right, total, sems):
        self.n, self.chunk, self.owner = n, chunk, n // 2 - 1
        self.send, self.from_left, self.from_right, self.total, self.sems = send, from_left, from_right, total, sems

    def at(self, half, k):
        p = lax.axis_index("tensor")
        rows = pl.ds(pl.multiple_of((2 * k + half) * self.chunk, self.chunk), self.chunk)
        q = p if half == 0 else self.n - 1 - p
        return q, p + 1 - 2 * half, p - 1 + 2 * half, rows

    def copy(self, half, k, kind, source, target, recv, device, rows):
        return pltpu.make_async_remote_copy(
            src_ref=source.at[rows, :], dst_ref=target.at[rows, :], send_sem=self.sems.at[kind, half, k],
            recv_sem=self.sems.at[recv, half, k], device_id={"tensor": device}, device_id_type=MESH)

    def inward_left(self, half, k):
        q, right, left, rows = self.at(half, k)
        return self.copy(half, k, 0, self.send, self.from_right, 2, left, rows)

    def inward_right(self, half, k):
        q, right, left, rows = self.at(half, k)
        return self.copy(half, k, 0, self.send, self.from_left, 1, right, rows)

    def outward_right(self, half, k):
        q, right, left, rows = self.at(half, k)
        return self.copy(half, k, 3, self.total, self.total, 5, right, rows)

    def outward_left(self, half, k):
        q, right, left, rows = self.at(half, k)
        return self.copy(half, k, 4, self.total, self.total, 5, left, rows)

    def edge(self, half, k):
        q = self.at(half, k)[0]

        @pl.when(q == self.n - 1)
        def _():
            self.inward_left(half, k).start()
        if self.owner > 0:
            @pl.when(q == 0)
            def _():
                self.inward_right(half, k).start()

    def mid(self, half, k):
        n, o = self.n, self.owner
        q, right, left, rows = self.at(half, k)
        if n - 1 - o > 1:
            @pl.when((q > o) & (q < n - 1))
            def _():
                self.inward_left(half, k).wait_recv()
                self.send[rows, :] = (self.send[rows, :].astype(F32) + self.from_right[rows, :].astype(F32)).astype(BF)
                self.inward_left(half, k).start()
        if o > 1:
            @pl.when((q < o) & (q > 0))
            def _():
                self.inward_right(half, k).wait_recv()
                self.send[rows, :] = (self.send[rows, :].astype(F32) + self.from_left[rows, :].astype(F32)).astype(BF)
                self.inward_right(half, k).start()

    def own(self, half, k):
        o = self.owner
        q, right, left, rows = self.at(half, k)

        @pl.when(q == o)
        def _():
            self.inward_left(half, k).wait_recv()
            total = self.send[rows, :].astype(F32) + self.from_right[rows, :].astype(F32)
            if o > 0:
                self.inward_right(half, k).wait_recv()
                total = total + self.from_left[rows, :].astype(F32)
            self.total[rows, :] = total.astype(BF)
            self.outward_right(half, k).start()
            if o > 0:
                self.outward_left(half, k).start()

    def forward(self, half, k):
        n, o = self.n, self.owner
        q = self.at(half, k)[0]

        @pl.when(q > o)
        def _():
            self.outward_right(half, k).wait_recv()

            @pl.when(q < n - 1)
            def _():
                self.outward_right(half, k).start()
        if o > 0:
            @pl.when(q < o)
            def _():
                self.outward_left(half, k).wait_recv()

                @pl.when(q > 0)
                def _():
                    self.outward_left(half, k).start()

    def drain(self, half, k):
        n, o = self.n, self.owner
        q = self.at(half, k)[0]

        @pl.when(q != o)
        def _():
            self.inward_left(half, k).wait_send()

        @pl.when((q >= o) & (q < n - 1))
        def _():
            self.outward_right(half, k).wait_send()
        if o > 0:
            @pl.when((q <= o) & (q > 0))
            def _():
                self.outward_left(half, k).wait_send()


def greet_line(n):
    p = lax.axis_index("tensor")
    barrier = pltpu.get_barrier_semaphore()

    @pl.when(p > 0)
    def _():
        pl.semaphore_signal(barrier, inc=1, device_id={"tensor": p - 1}, device_id_type=MESH)

    @pl.when(p < n - 1)
    def _():
        pl.semaphore_signal(barrier, inc=1, device_id={"tensor": p + 1}, device_id_type=MESH)

    inner = (p > 0) & (p < n - 1)

    @pl.when(inner)
    def _():
        pl.semaphore_wait(barrier, 2)

    @pl.when(jnp.logical_not(inner))
    def _():
        pl.semaphore_wait(barrier, 1)


def standardize(values):
    center = values - jnp.mean(values, axis=1, keepdims=True)
    rate = lax.rsqrt(jnp.mean(center * center, axis=1, keepdims=True) + eps_norm)
    return center * rate, rate


def norm_back(grad, unit, rate, gain):
    scaled = grad * gain
    return rate * (scaled - jnp.mean(scaled, axis=1, keepdims=True) - unit * jnp.mean(scaled * unit, axis=1, keepdims=True))


def middle_kernel(n, ctx, rows, wo_t, norms, cot_hbm, up_hbm, down_hbm, outputs, d_first, d_ctx, g_up, g_down, g_out, g_norm,
                  cot, up, down, low, act, d_ffn, d_hid, d_br, unit, slope, d_sec, rates, sums, load_sems, *line_refs):
    R, D = rows.shape
    chunk = R // (2 * ROUNDS)
    pair = 2 * chunk
    loads = [pltpu.make_async_copy(a, b, load_sems.at[i]) for i, (a, b) in
             enumerate([(up_hbm, up), (down_hbm, down), (cot_hbm, cot)])]
    for load in loads:
        load.start()
    lines = [Line(n, chunk, *line_refs[5 * i:5 * i + 5]) for i in range(3)]
    greet_line(n)
    sums[...] = jnp.zeros_like(sums)

    def add_sum(i, values):
        sums[8 * i:8 * i + 8, :] += jnp.sum(values.reshape(pair // 8, 8, D), axis=0)

    def pair_rows(k):
        return pl.ds(pl.multiple_of(k * pair, pair), pair)

    def open_first(k):
        r = pair_rows(k)
        lines[0].send[r, :] = dotf(ctx[r, :], wo_t[...], 1, 1).astype(BF)

    def first_to_second(k):
        r = pair_rows(k)
        u, rate = standardize(rows[r, :].astype(F32) + lines[0].total[r, :].astype(F32))
        unit[r, :] = u
        rates[r, :] = jnp.broadcast_to(rate, (pair, 128))
        nl = (u * norms[0:1, :] + norms[1:2, :]).astype(BF)
        low[r, :] = nl
        hidden = dotf(nl, up[...], 1, 0)
        half_cdf = 0.5 * (1.0 + lax.erf(hidden * 0.7071067811865476))
        slope[r, :] = half_cdf + hidden * (jnp.exp(-0.5 * hidden * hidden) * 0.3989422804014327)
        a = (hidden * half_cdf).astype(BF)
        act[r, :] = a
        lines[1].send[r, :] = dotf(a, down[...], 1, 1).astype(BF)

    def second_to_third(k):
        r = pair_rows(k)
        u, rate = standardize(unit[r, :] * norms[0:1, :] + norms[1:2, :] + lines[1].total[r, :].astype(F32))
        outputs[r, :] = (u * norms[2:3, :] + norms[3:4, :]).astype(BF)
        g = cot[r, :].astype(F32)
        add_sum(2, g * u)
        add_sum(3, g)
        ds = norm_back(g, u, rate, norms[2:3, :])
        d_sec[r, :] = ds
        dl = ds.astype(BF)
        d_ffn[r, :] = dl
        dh = (dotf(dl, down[...], 1, 0) * slope[r, :]).astype(BF)
        d_hid[r, :] = dh
        lines[2].send[r, :] = dotf(dh, up[...], 1, 1).astype(BF)

    def close_third(k):
        r = pair_rows(k)
        g = d_sec[r, :] + lines[2].total[r, :].astype(F32)
        u = unit[r, :]
        add_sum(0, g * u)
        add_sum(1, g)
        d1 = norm_back(g, u, rates[r, 0:1], norms[0:1, :])
        d_first[r, :] = d1
        db = d1.astype(BF)
        d_br[r, :] = db
        d_ctx[r, :] = dotf(db, wo_t[...], 1, 0).astype(BF)

    def weight_grad(out, left, right):
        width = min(256, D)

        def tile(i, _):
            c = pl.ds(pl.multiple_of(i * width, width), width)
            out[c, :] = dotf(left[:, c], right[...], 0, 0).astype(BF)
            return 0
        lax.fori_loop(0, D // width, tile, 0)

    def when_valid(t, lag, body):
        @pl.when((t >= lag) & (t < lag + ROUNDS))
        def _():
            body(t - lag)

    def both(stage):
        def run(k):
            stage(0, k)
            stage(1, k)
        return run

    def start(line, body):
        def run(k):
            body(k)
            line.edge(0, k)
            line.edge(1, k)
        return run

    def step(t, _):
        for i in (2, 1, 0):
            for lag, stage in ((8, lines[i].forward), (6, lines[i].own), (4, lines[i].mid)):
                when_valid(t, 8 * i + lag, both(stage))
        when_valid(t, 24, close_third)
        when_valid(t, 16, start(lines[2], second_to_third))
        when_valid(t, 8, start(lines[1], first_to_second))
        when_valid(t, 0, start(lines[0], open_first))

        @pl.when(t == 7)
        def _():
            for load in loads:
                load.wait()

        @pl.when(t == 16 + ROUNDS)
        def _():
            weight_grad(g_down, d_ffn, act)

        @pl.when(t == 17 + ROUNDS)
        def _():
            weight_grad(g_up, low, d_hid)
        return 0

    lax.fori_loop(0, ROUNDS + 24, step, 0)
    weight_grad(g_out, d_br, ctx)
    for i in range(4):
        g_norm[i:i + 1, :] = jnp.sum(sums[8 * i:8 * i + 8, :], axis=0, keepdims=True)
    g_norm[4:8, :] = jnp.zeros((4, D), F32)

    def finish(k, _):
        for line in lines:
            line.drain(0, k)
            line.drain(1, k)
        return 0
    lax.fori_loop(0, ROUNDS, finish, 0)


def middle(n, ctx, rows, wo_t, norms, cot, up, down):
    R, D = rows.shape
    Wd, F = wo_t.shape[1], up.shape[1]
    vmem, hbm = pl.BlockSpec(memory_space=pltpu.VMEM), pl.BlockSpec(memory_space=pl.ANY)
    line = [pltpu.VMEM((R, D), BF)] * 4 + [pltpu.SemaphoreType.DMA((6, 2, ROUNDS))]
    shape = jax.ShapeDtypeStruct
    return pl.pallas_call(
        partial(middle_kernel, n),
        in_specs=[vmem] * 4 + [hbm] * 3,
        out_specs=[vmem] * 7,
        out_shape=[shape((R, D), BF), shape((R, D), F32), shape((R, Wd), BF), shape((D, F), BF), shape((D, F), BF),
                   shape((D, Wd), BF), shape((8, D), F32)],
        scratch_shapes=[pltpu.VMEM((R, D), BF), pltpu.VMEM((D, F), BF), pltpu.VMEM((D, F), BF), pltpu.VMEM((R, D), BF),
                        pltpu.VMEM((R, F), BF), pltpu.VMEM((R, D), BF), pltpu.VMEM((R, F), BF), pltpu.VMEM((R, D), BF),
                        pltpu.VMEM((R, D), F32), pltpu.VMEM((R, F), F32), pltpu.VMEM((R, D), F32), pltpu.VMEM((R, 128), F32),
                        pltpu.VMEM((32, D), F32), pltpu.SemaphoreType.DMA((3,))] + line * 3,
        compiler_params=pltpu.CompilerParams(collective_id=1, has_side_effects=True),
        name="middle",
        cost_estimate=pl.CostEstimate(flops=12 * R * D * F, bytes_accessed=16 * R * D, transcendentals=2 * R * F),
    )(ctx, rows, wo_t, norms, cot, up, down)


def plane_peers():
    s, c = lax.axis_index("shard"), lax.axis_index("context")
    near = [s, s + 1 - 2 * (s % 2), (s + 2) % 4, 3 - s]
    return near, c


def greet_plane():
    near, c = plane_peers()
    barrier = pltpu.get_barrier_semaphore()
    pl.semaphore_signal(barrier, inc=1, device_id={"context": 1 - c}, device_id_type=MESH)
    for j in (1, 2):
        pl.semaphore_signal(barrier, inc=1, device_id={"shard": near[j]}, device_id_type=MESH)
    pl.semaphore_wait(barrier, 3)


class Scatter:
    def __init__(self, mats, partner_in, acc, corner_in, came, sems, loads=None):
        self.mats, self.partner_in, self.acc, self.corner_in, self.came = mats, partner_in, acc, corner_in, came
        self.sems, self.loads = sems, loads
        self.own = corner_in.shape[1]

    def block(self, j):
        return pl.ds(j * self.own, self.own)

    def source(self, side, j, other):
        near, c = plane_peers()
        core = 1 - c if other else c
        return self.mats[side].at[pl.ds(pl.multiple_of((2 * near[j] + core) * self.own, self.own), self.own), :]

    def to_partner(self, side, j):
        c = lax.axis_index("context")
        return pltpu.make_async_remote_copy(
            src_ref=self.source(side, j, True), dst_ref=self.partner_in.at[side, self.block(j), :],
            send_sem=self.sems.at[0, side, j], recv_sem=self.sems.at[1, side, j], device_id={"context": 1 - c}, device_id_type=MESH)

    def load(self, side, j):
        return pltpu.make_async_copy(self.source(side, j, False), self.acc.at[side, self.block(j), :], self.loads.at[side, j])

    def hop(self, side, j, axis, target, kind):
        near, _ = plane_peers()
        return pltpu.make_async_remote_copy(
            src_ref=self.acc.at[side, self.block(j), :], dst_ref=target, send_sem=self.sems.at[2, side, kind],
            recv_sem=self.sems.at[3, side, kind], device_id={"shard": near[axis]}, device_id_type=MESH)

    def corner(self, side):
        return self.hop(side, 3, 1 + side, self.corner_in.at[side], 0)

    def early(self, side):
        return self.hop(side, 1 + side, 1 + side, self.came.at[side, 0], 1)

    def late(self, side):
        return self.hop(side, 2 - side, 2 - side, self.came.at[side, 1], 2)

    def begin(self, side):
        for j in (3, 1, 2, 0):
            self.to_partner(side, j).start()
            if self.loads is not None:
                self.load(side, j).start()

    def add_partner(self, side, j):
        self.to_partner(side, j).wait_recv()
        if self.loads is not None:
            self.load(side, j).wait()
            mine = self.acc[side, self.block(j), :]
        else:
            mine = self.source(side, j, False)[...]
        self.acc[side, self.block(j), :] = (mine.astype(F32) + self.partner_in[side, self.block(j), :].astype(F32)).astype(BF)

    def spread(self, side):
        self.add_partner(side, 3)
        self.corner(side).start()
        self.add_partner(side, 1 + side)
        self.early(side).start()
        self.add_partner(side, 2 - side)
        self.add_partner(side, 0)

    def turn(self, side):
        self.corner(side).wait_recv()
        b = self.block(2 - side)
        self.acc[side, b, :] = (self.acc[side, b, :].astype(F32) + self.corner_in[side].astype(F32)).astype(BF)
        self.late(side).start()

    def result(self, side):
        self.early(side).wait_recv()
        self.late(side).wait_recv()
        return (self.acc[side, self.block(0), :].astype(F32) + self.came[side, 0].astype(F32) + self.came[side, 1].astype(F32))

    def drain(self, side):
        for j in range(4):
            self.to_partner(side, j).wait_send()
        self.corner(side).wait_send()
        self.early(side).wait_send()
        self.late(side).wait_send()


def scatter_scratch(own, width, load):
    shapes = [pltpu.VMEM((2, 4 * own, width), BF), pltpu.VMEM((2, 4 * own, width), BF), pltpu.VMEM((2, own, width), BF),
              pltpu.VMEM((2, 2, own, width), BF), pltpu.SemaphoreType.DMA((4, 2, 4))]
    return shapes + ([pltpu.SemaphoreType.DMA((2, 4))] if load else [])


def attend_back_scatter_kernel(*refs, scale):
    ins, (g_up, g_down), outs, (o_up, o_down), scratch, shared = refs[:7], refs[7:9], refs[9:14], refs[14:16], refs[16:19], refs[19:]
    job = Scatter((g_up, g_down), *shared)
    step, last = pl.program_id(0), pl.num_programs(0) - 1

    @pl.when(step == 0)
    def _():
        greet_plane()
        job.begin(0)
        job.begin(1)

    def between(half):
        if half == 0:
            @pl.when(step == 0)
            def _():
                job.spread(0)
                job.spread(1)
        else:
            @pl.when(step == 0)
            def _():
                job.turn(0)
                job.turn(1)

    attend_back_kernel(*ins, *outs, *scratch, scale=scale, between=between)

    @pl.when(step == last)
    def _():
        o_up[...] = job.result(0)
        o_down[...] = job.result(1).T
        job.drain(0)
        job.drain(1)


def attend_back_scatter(q, k, v, kd, pq, p, dc, g_up, g_down, scale):
    S, L, Wd = q.shape
    T = k.shape[1]
    W = kd.shape[0]
    D, F = g_up.shape
    own, pairs = D // 8, Wd // 128
    row = lambda n: pl.BlockSpec((1, n, 128), lambda h, s: (s, 0, h))
    tab = pl.BlockSpec((W, 128), lambda h, s: (0, h))
    hbm = pl.BlockSpec(memory_space=pl.ANY)
    fixed = lambda *shape: pl.BlockSpec(shape, lambda h, s: (0, 0))
    return pl.pallas_call(
        partial(attend_back_scatter_kernel, scale=scale), grid=(pairs, S),
        in_specs=[row(L), row(T), row(T), tab, tab, pl.BlockSpec((1, 2, L, T), lambda h, s: (s, h, 0, 0)), row(L), hbm, hbm],
        out_specs=[row(L), row(T), row(T), tab, tab, fixed(own, F), fixed(F, own)],
        out_shape=[jax.ShapeDtypeStruct((S, n, Wd), BF) for n in (L, T, T)] + [jax.ShapeDtypeStruct((W, Wd), F32)] * 2
        + [jax.ShapeDtypeStruct((own, F), F32), jax.ShapeDtypeStruct((F, own), F32)],
        scratch_shapes=[pltpu.VMEM((L, T), BF), pltpu.VMEM((L, T), BF), pltpu.VMEM((T, HD), F32)] + scatter_scratch(own, F, True),
        compiler_params=pltpu.CompilerParams(collective_id=3, has_side_effects=True),
        name="attend_back",
        cost_estimate=pl.CostEstimate(flops=int(32 * S * L * T * Wd), bytes_accessed=int(S * L * T * Wd // HD * 4), transcendentals=0),
    )(q, k, v, kd, pq, p, dc, g_up, g_down)


def tail_kernel(n, dq, dk, dv, wqkv, rows, d_first, pos_t, to_row, from_row, dkd, dpq, g_out, g_norm,
                grad_in, o_q, o_k, o_v, o_out, o_pos, o_norm,
                k_in, v_in, dqkv, d_pos, g_left, g_right, norm_in, swap_sems, norm_sems, *refs):
    L, Wd = dq.shape
    D, B = pos_t.shape
    W = to_row.shape[1]
    own = D // 8
    chunk = L // (2 * ROUNDS)
    pair = 2 * chunk
    line = Line(n, chunk, *refs[:5])
    small = Line(n, own // 2, *refs[5:10])
    job = Scatter((g_left, g_right), *refs[10:])
    near, c = plane_peers()
    p = lax.axis_index("tensor")
    barrier = pltpu.get_barrier_semaphore()
    for j in range(4):
        for core in (c, 1 - c):
            if j > 0 or core is not c:
                pl.semaphore_signal(barrier, inc=1, device_id={"shard": near[j], "context": core}, device_id_type=MESH)

    @pl.when(p > 0)
    def _():
        pl.semaphore_signal(barrier, inc=1, device_id={"tensor": p - 1}, device_id_type=MESH)

    @pl.when(p < n - 1)
    def _():
        pl.semaphore_signal(barrier, inc=1, device_id={"tensor": p + 1}, device_id_type=MESH)
    inner = (p > 0) & (p < n - 1)

    @pl.when(inner)
    def _():
        pl.semaphore_wait(barrier, 9)

    @pl.when(jnp.logical_not(inner))
    def _():
        pl.semaphore_wait(barrier, 8)

    def swap(i, source, target):
        part = pl.ds(pl.multiple_of((1 - c) * L, L), L)
        return pltpu.make_async_remote_copy(src_ref=source.at[part, :], dst_ref=target, send_sem=swap_sems.at[0, i],
                                            recv_sem=swap_sems.at[1, i], device_id={"context": 1 - c}, device_id_type=MESH)
    swaps = [swap(0, dk, k_in), swap(1, dv, v_in)]
    for s in swaps:
        s.start()
    pieces = []
    for j in range(4):
        for other in range(2):
            core = c if other == 0 else 1 - c
            if j == 0 and other == 0:
                continue
            i = 2 * j + other
            lanes = pl.ds(pl.multiple_of((2 * near[j] + core) * own, own), own)
            pieces.append(pltpu.make_async_remote_copy(
                src_ref=g_norm.at[:, lanes], dst_ref=norm_in.at[i], send_sem=norm_sems.at[0, i], recv_sem=norm_sems.at[1, i],
                device_id={"shard": near[j], "context": core}, device_id_type=MESH))
    for piece in pieces:
        piece.start()

    ids = lax.broadcasted_iota(jnp.int32, (B, W), 0)
    d_pos[:, :Wd] = dotf((ids == from_row[...]).astype(F32).astype(BF), dpq[...].astype(BF), 1, 0).astype(BF)
    d_pos[:, Wd:] = dotf((ids == to_row[...]).astype(F32).astype(BF), dkd[...].astype(BF), 1, 0).astype(BF)
    g_right[:, :Wd] = g_out[...]
    width = 256

    def right_tile(i, _):
        r = pl.ds(pl.multiple_of(i * width, width), width)
        g_right[r, Wd:] = dotf(wqkv[r, :2 * Wd], d_pos[...], 1, 1).astype(BF)
        return 0
    lax.fori_loop(0, D // width, right_tile, 0)
    job.begin(1)
    here = pl.ds(pl.multiple_of(c * L, L), L)
    dqkv[:, :Wd] = dq[...]
    for s, mine, got, at in ((swaps[0], dk, k_in, Wd), (swaps[1], dv, v_in, 2 * Wd)):
        s.wait_recv()
        dqkv[:, at:at + Wd] = (mine[here, :].astype(F32) + got[...].astype(F32)).astype(BF)

    def pair_rows(k):
        return pl.ds(pl.multiple_of(k * pair, pair), pair)

    def produce(k, _):
        r = pair_rows(k)
        line.send[r, :] = dotf(dqkv[r, :], wqkv[...], 1, 1).astype(BF)
        line.edge(0, k)
        line.edge(1, k)
        return 0
    lax.fori_loop(0, ROUNDS, produce, 0)

    def left_tile(i, _):
        r = pl.ds(pl.multiple_of(i * width, width), width)
        g = dotf(rows[:, r], dqkv[...], 0, 0)
        g_left[r, :2 * Wd] = (g[:, :2 * Wd] + dotf(pos_t[r, :], d_pos[...], 1, 0)).astype(BF)
        g_left[r, 2 * Wd:] = g[:, 2 * Wd:].astype(BF)
        return 0
    lax.fori_loop(0, D // width, left_tile, 0)
    job.begin(0)
    job.spread(1)

    def step(t, _):
        for lag, stage in ((4, line.forward), (2, line.own), (0, line.mid)):
            @pl.when((t >= lag) & (t < lag + ROUNDS))
            def _():
                stage(0, t - lag)
                stage(1, t - lag)

        @pl.when((t >= 4) & (t < 4 + ROUNDS))
        def _():
            r = pair_rows(t - 4)
            grad_in[r, :] = (d_first[r, :] + line.total[r, :].astype(F32)).astype(BF)

        @pl.when(t == 0)
        def _():
            job.spread(0)

        @pl.when(t == 2)
        def _():
            job.turn(1)
            job.turn(0)

        @pl.when(t == 6)
        def _():
            right = job.result(1)
            o_out[...] = right[:, :Wd].T
            small.send[...] = right[:, Wd:].astype(BF)
            small.edge(0, 0)
            small.edge(1, 0)

        @pl.when(t == 7)
        def _():
            left = job.result(0)
            o_q[...] = left[:, :Wd]
            o_k[...] = left[:, Wd:2 * Wd]
            o_v[...] = left[:, 2 * Wd:]

        for at, stage in ((8, small.mid), (9, small.own), (11, small.forward)):
            @pl.when(t == at)
            def _():
                stage(0, 0)
                stage(1, 0)
        return 0
    lax.fori_loop(0, ROUNDS + 4, step, 0)
    o_pos[...] = small.total[...].astype(F32).T
    lanes = pl.ds(pl.multiple_of((2 * near[0] + c) * own, own), own)
    total = g_norm[:, lanes]
    for piece in pieces:
        piece.wait_recv()
    for i in range(1, 8):
        total = total + norm_in[i]
    o_norm[...] = total

    def finish(k, _):
        line.drain(0, k)
        line.drain(1, k)
        return 0
    lax.fori_loop(0, ROUNDS, finish, 0)
    small.drain(0, 0)
    small.drain(1, 0)
    job.drain(0)
    job.drain(1)
    for copy in swaps + pieces:
        copy.wait_send()


def tail(n, dq, dk, dv, wqkv, rows, d_first, pos_t, to_row, from_row, dkd, dpq, g_out, g_norm):
    L, Wd = dq.shape
    D, B = pos_t.shape
    own = D // 8
    vmem = pl.BlockSpec(memory_space=pltpu.VMEM)
    shape = jax.ShapeDtypeStruct
    line = [pltpu.VMEM((L, D), BF)] * 4 + [pltpu.SemaphoreType.DMA((6, 2, ROUNDS))]
    small = [pltpu.VMEM((own, B), BF)] * 4 + [pltpu.SemaphoreType.DMA((6, 2, 1))]
    return pl.pallas_call(
        partial(tail_kernel, n),
        in_specs=[vmem] * 13, out_specs=[vmem] * 7,
        out_shape=[shape((L, D), BF)] + [shape((own, Wd), F32)] * 3 + [shape((Wd, own), F32), shape((B, own), F32), shape((8, own), F32)],
        scratch_shapes=[pltpu.VMEM((L, Wd), BF), pltpu.VMEM((L, Wd), BF), pltpu.VMEM((L, 3 * Wd), BF), pltpu.VMEM((B, 2 * Wd), BF),
                        pltpu.VMEM((D, 3 * Wd), BF), pltpu.VMEM((D, Wd + B), BF), pltpu.VMEM((8, 8, own), F32),
                        pltpu.SemaphoreType.DMA((2, 2)), pltpu.SemaphoreType.DMA((2, 8))] + line + small
        + scatter_scratch(own, 3 * Wd, False),
        compiler_params=pltpu.CompilerParams(collective_id=4, has_side_effects=True),
        name="tail",
        cost_estimate=pl.CostEstimate(flops=8 * L * D * 3 * Wd, bytes_accessed=16 * L * D, transcendentals=0),
    )(dq, dk, dv, wqkv, rows, d_first, pos_t, to_row, from_row, dkd, dpq, g_out, g_norm)


def split_columns(packed, widths):
    at, out = 0, []
    for width in widths:
        out.append(packed[:, at:at + width])
        at += width
    return out


def local(inputs, cotangent, segments, buckets, w_query, w_key, w_value, w_output, w_up, w_down,
          positions, gain_attn, bias_attn, gain_ffn, bias_ffn):
    S, L, D = inputs.shape
    T = segments.shape[1]
    Wd = w_query.shape[1]
    F = w_up.shape[1]
    B = positions.shape[0]
    scale = 1.0 / math.sqrt(3 * HD)
    first = lax.axis_index("context") * L
    W = T + L
    own = w_query.shape[0]
    norms = jnp.stack([gain_attn, bias_attn, gain_ffn, bias_ffn], axis=1)
    norms = jnp.pad(norms, ((0, 0), (0, 124)))
    pack = jnp.concatenate([w_query, w_key, w_value, w_output.T, positions.T, norms], axis=1)
    pack = lax.all_gather(pack, BOTH, axis=0, tiled=True)
    wq, wk, wv, wo_t, pos_t, norms = split_columns(pack, (Wd, Wd, Wd, Wd, B, 128))
    ffn = lax.all_gather(jnp.concatenate([w_up, w_down.T], axis=1), BOTH, axis=0, tiled=True)
    up, down_t = split_columns(ffn, (F, F))
    norms = jnp.pad(norms[:, :4].astype(F32).T, ((0, 4), (0, 0)))
    rows = inputs.reshape(S * L, D)
    wqkv = pack[:, :3 * Wd]
    qkv = dotf(rows, wqkv, 1, 0).astype(BF)
    q, k, v = [x.reshape(S, L, Wd) for x in split_columns(qkv, (Wd, Wd, Wd))]
    k, v = split_last(lax.all_gather(jnp.concatenate([k, v], axis=2), "context", axis=1, tiled=True), Wd)
    pos_qk = dotf(pos_t, jnp.concatenate([wq, wk], axis=1), 0, 0).astype(BF)
    flipped = jnp.concatenate([buckets[::-1], buckets[:1]])
    to = lax.dynamic_slice_in_dim(flipped, T - L - first, W, 0)
    fro = lax.dynamic_slice_in_dim(flipped, first, W, 0)
    ids = jnp.arange(B, dtype=jnp.int32)
    pick_to = (to[:, None] == ids[None]).astype(BF)
    pick_from = (fro[:, None] == ids[None]).astype(BF)
    kd = dotf(pick_to, pos_qk[:, Wd:], 1, 0).astype(BF)
    pq = dotf(pick_from, pos_qk[:, :Wd], 1, 0).astype(BF)
    seg_here = lax.dynamic_slice_in_dim(segments, first, L, 1)[:, :, None]
    ctx, probs = attend(q, k, v, kd, pq, seg_here, segments[:, None, :], scale)
    ctx_rows = ctx.reshape(S * L, Wd)
    outputs, d_first, d_ctx, g_up, g_down_t, g_out_t, g_norm = middle(
        lax.axis_size("tensor"), ctx_rows, rows, wo_t, norms, cotangent.reshape(S * L, D), up, down_t)
    outputs = outputs.reshape(inputs.shape)
    f = lambda x: x.astype(F32)
    if (lax.axis_size("shard"), lax.axis_size("context"), S, own * 8, 3 * Wd) == (4, 2, 1, D, Wd + B):
        dq, dk, dv, dkd, dpq, g_up, g_down = attend_back_scatter(q, k, v, kd, pq, probs, d_ctx.reshape(S, L, Wd), g_up, g_down_t, scale)
        grad_inputs, g_q, g_k, g_v, g_o, g_p, g_n = tail(
            lax.axis_size("tensor"), dq[0], dk[0], dv[0], wqkv, rows, d_first, pos_t, to[None], fro[None], dkd, dpq, g_out_t, g_norm)
        return (outputs, grad_inputs.reshape(inputs.shape), g_q, g_k, g_v, g_o, g_up, g_down, g_p, g_n[0], g_n[1], g_n[2], g_n[3])
    scatter = partial(lax.psum_scatter, axis_name=BOTH, scatter_dimension=0, tiled=True)
    g_ffn = scatter(jnp.concatenate([g_up, g_down_t], axis=1))
    dq, dk, dv, dkd, dpq = attend_back(q, k, v, kd, pq, probs, d_ctx.reshape(S, L, Wd), scale)
    dkv = lax.psum_scatter(jnp.concatenate([dk, dv], axis=2), "context", scatter_dimension=1, tiled=True)
    dqkv = jnp.concatenate([dq, dkv], axis=2).reshape(S * L, 3 * Wd)
    weights = jnp.concatenate([wq, wk, wv], axis=1)
    d_in = lax.psum(dotf(dqkv, weights, 1, 1).astype(BF), "tensor").astype(F32)
    grad_inputs = (d_first + d_in).astype(BF).reshape(inputs.shape)
    d_pos_key = dotf(pick_to, dkd.astype(BF), 0, 0)
    d_pos_query = dotf(pick_from, dpq.astype(BF), 0, 0)
    d_pos = jnp.concatenate([d_pos_query, d_pos_key], axis=1).astype(BF)
    g_qkv = dotf(rows, dqkv, 0, 0)
    g_pos_t = dotf(jnp.concatenate([wq, wk], axis=1), d_pos, 1, 1)
    g_qk = g_qkv[:, :2 * Wd] + dotf(pos_t, d_pos, 1, 0)
    g_norm = jnp.pad(g_norm.T, ((0, 0), (0, 120)))
    pack = jnp.concatenate([x.astype(BF) for x in (g_qk, g_qkv[:, 2 * Wd:], g_out_t, g_pos_t, g_norm)], axis=1)
    g_q, g_k, g_v, g_o, g_p, g_n = split_columns(scatter(pack), (Wd, Wd, Wd, Wd, B, 128))
    g_p = lax.psum(g_p, "tensor")
    return (outputs, grad_inputs, f(g_q), f(g_k), f(g_v), f(g_o).T, f(g_ffn[:, :F]), f(g_ffn[:, F:]).T, f(g_p).T,
            f(g_n[:, 0]), f(g_n[:, 1]), f(g_n[:, 2]), f(g_n[:, 3]))


def split_last(packed, width):
    return packed[..., :width], packed[..., width:]


def solution(mesh):
    P = jax.sharding.PartitionSpec
    act, row, col, vec = P("shard", "context", None), P(BOTH, "tensor"), P("tensor", BOTH), P(BOTH)
    return jax.shard_map(local, mesh=mesh,
        in_specs=(act, act, P("shard", None), P(), row, row, row, col, row, col, P(None, BOTH), vec, vec, vec, vec),
        out_specs=(act, act, row, row, row, col, row, col, P(None, BOTH), vec, vec, vec, vec),
        check_vma=False)
```

```python
import functools
import math
from functools import partial
import jax, jax.numpy as jnp
from jax import lax
from jax.experimental import pallas as pl
from jax.experimental.pallas import tpu as pltpu
HD=64
NEG=-1000000000.0
TILE=128
F32=jnp.float32
BF=jnp.bfloat16

def dotf(a,b,ca,cb,precision=None):
    return lax.dot_general(a,b,(((ca,),(cb,)),((),())),preferred_element_type=F32,precision=precision)

def reversal(n,dtype):
    r=lax.broadcasted_iota(jnp.int32,(n,n),0); c=lax.broadcasted_iota(jnp.int32,(n,n),1)
    return (r+c==n-1).astype(F32).astype(dtype)

def attend_kernel(q_ref,k_ref,v_ref,kd_ref,pq_ref,sq_ref,sk_ref,ctx_ref,p_ref,st_ref,*,scale,between=None):
    rows=q_ref.shape[1]; total=k_ref.shape[1]; tile=min(TILE,rows)
    same_row=sk_ref[0]
    for half in range(2):
        cols=slice(half*HD,(half+1)*HD)
        q=q_ref[0][:,cols]; k=k_ref[0][:,cols]; v=v_ref[0][:,cols]
        kd=kd_ref[:,cols]; pq=pq_ref[:,cols]
        for j0 in range(0,total,TILE):
            width=rows+TILE; start=total-j0-TILE
            b=dotf(k[j0:j0+TILE],pq[start:start+width],1,1)
            b=pltpu.roll(b,width-TILE+1,axis=1,stride=1,stride_axis=0)[:,:rows]
            st_ref[:,j0:j0+TILE]=b.T
        for i0 in range(0,rows,tile):
            width=total+tile; start=rows-i0-tile
            qt=q[i0:i0+tile]
            a=dotf(qt,kd[start:start+width],1,1)
            a=pltpu.roll(a,width-tile+1,axis=1,stride=1,stride_axis=0)[:,:total]
            raw=dotf(qt,k,1,1)+a+st_ref[i0:i0+tile,:]
            s=jnp.where(sq_ref[0][i0:i0+tile]==same_row,raw*scale,NEG)
            e=jnp.exp(s-jnp.max(s,axis=1,keepdims=True))
            p=e*(1.0/jnp.sum(e,axis=1,keepdims=True))
            p_ref[0,half,i0:i0+tile,:]=p
            ctx_ref[0,i0:i0+tile,cols]=dotf(p.astype(BF),v,1,0).astype(BF)
        if between is not None:
            between(half)

def attend_back_kernel(q_ref,k_ref,v_ref,kd_ref,pq_ref,p_ref,dc_ref,dq_ref,dk_ref,dv_ref,dkd_ref,dpq_ref,ds_ref,pl_ref,dkt_ref,*,scale,between=None):
    rows=q_ref.shape[1]; total=k_ref.shape[1]; tile=min(TILE,rows)
    @pl.when(pl.program_id(1)==0)
    def _():
        dkd_ref[...]=jnp.zeros_like(dkd_ref)
        dpq_ref[...]=jnp.zeros_like(dpq_ref)
    flip_t=reversal(tile,BF); flip_j=reversal(TILE,BF)
    hi=lax.Precision.HIGHEST
    for half in range(2):
        cols=slice(half*HD,(half+1)*HD)
        q=q_ref[0][:,cols]; k=k_ref[0][:,cols]; v=v_ref[0][:,cols]; dc=dc_ref[0][:,cols]
        kd=kd_ref[:,cols]; pq=pq_ref[:,cols]
        for i0 in range(0,rows,tile):
            width=total+tile; start=rows-i0-tile
            p=p_ref[0,half,i0:i0+tile,:]
            dp=dotf(dc[i0:i0+tile],v,1,1)
            inner=jnp.sum(p*dp,axis=1,keepdims=True)
            ds=(p*(dp-inner)*scale).astype(BF)
            ds_ref[i0:i0+tile,:]=ds
            pl_ref[i0:i0+tile,:]=p.astype(BF)
            rev=dotf(flip_t,ds,1,0).astype(BF)
            rev=jnp.concatenate([rev,jnp.zeros((tile,tile),BF)],axis=1)
            rev=pltpu.roll(rev,0,axis=1,stride=1,stride_axis=0)
            qrev=dotf(flip_t,q[i0:i0+tile],1,0).astype(BF)
            dqr=dotf(rev,kd[start:start+width],1,0)
            dq=dotf(ds,k,1,0)+dotf(flip_t.astype(F32),dqr,1,0,hi)
            dq_ref[0,i0:i0+tile,cols]=dq.astype(BF)
            dkd_ref[start:start+width,cols]+=dotf(rev,qrev,0,0)
        dsf=ds_ref[...]
        dv_ref[0,:,cols]=dotf(pl_ref[...],dc,0,0).astype(BF)
        dkt_ref[...]=dotf(dsf,q,0,0)
        for j0 in range(0,total,TILE):
            width=rows+TILE; start=total-j0-TILE
            rev=dotf(flip_j,ds_ref[:,j0:j0+TILE],1,1).astype(BF)
            rev=jnp.concatenate([rev,jnp.zeros((TILE,TILE),BF)],axis=1)
            rev=pltpu.roll(rev,0,axis=1,stride=1,stride_axis=0)
            krev=dotf(flip_j,k[j0:j0+TILE],1,0).astype(BF)
            dkr=dotf(rev,pq[start:start+width],1,0)
            dk=dkt_ref[j0:j0+TILE,:]+dotf(flip_j.astype(F32),dkr,1,0,hi)
            dk_ref[0,j0:j0+TILE,cols]=dk.astype(BF)
            dpq_ref[start:start+width,cols]+=dotf(rev,krev,0,0)
        if between is not None:
            between(half)

def attend(q,k,v,kd,pq,sq,sk,scale):
    S,L,Wd=q.shape; T=k.shape[1]; W=kd.shape[0]; pairs=Wd//128
    row=lambda n:pl.BlockSpec((1,n,128),lambda s,h:(s,0,h))
    tab=pl.BlockSpec((W,128),lambda s,h:(0,h))
    return pl.pallas_call(functools.partial(attend_kernel,scale=scale),grid=(S,pairs),
      in_specs=[row(L),row(T),row(T),tab,tab,pl.BlockSpec((1,L,1),lambda s,h:(s,0,0)),pl.BlockSpec((1,1,T),lambda s,h:(s,0,0))],
      out_specs=[row(L),pl.BlockSpec((1,2,L,T),lambda s,h:(s,h,0,0))],
      out_shape=[jax.ShapeDtypeStruct((S,L,Wd),BF),jax.ShapeDtypeStruct((S,Wd//HD,L,T),F32)],
      scratch_shapes=[pltpu.VMEM((L,T),F32)],name="attend",
      cost_estimate=pl.CostEstimate(flops=int(16*S*L*T*Wd),bytes_accessed=int(S*L*T*Wd//HD*4),transcendentals=S*L*T*Wd//HD))(q,k,v,kd,pq,sq,sk)

def attend_back(q,k,v,kd,pq,p,dc,scale):
    S,L,Wd=q.shape; T=k.shape[1]; W=kd.shape[0]; pairs=Wd//128
    row=lambda n:pl.BlockSpec((1,n,128),lambda h,s:(s,0,h))
    tab=pl.BlockSpec((W,128),lambda h,s:(0,h))
    return pl.pallas_call(functools.partial(attend_back_kernel,scale=scale),grid=(pairs,S),
      in_specs=[row(L),row(T),row(T),tab,tab,pl.BlockSpec((1,2,L,T),lambda h,s:(s,h,0,0)),row(L)],
      out_specs=[row(L),row(T),row(T),tab,tab],
      out_shape=[jax.ShapeDtypeStruct((S,n,Wd),BF) for n in (L,T,T)]+[jax.ShapeDtypeStruct((W,Wd),F32)]*2,
      scratch_shapes=[pltpu.VMEM((L,T),BF),pltpu.VMEM((L,T),BF),pltpu.VMEM((T,HD),F32)],name="attend_back",
      cost_estimate=pl.CostEstimate(flops=int(32*S*L*T*Wd),bytes_accessed=int(S*L*T*Wd//HD*4),transcendentals=0))(q,k,v,kd,pq,p,dc)


BOTH = ("shard", "context")
eps_norm = 1e-06

MESH = pl.DeviceIdType.MESH
ROUNDS = 8


class Line:
    def __init__(self, n, chunk, send, from_left, from_right, total, sems):
        self.n, self.chunk, self.owner = n, chunk, n // 2 - 1
        self.send, self.from_left, self.from_right, self.total, self.sems = send, from_left, from_right, total, sems

    def at(self, half, k):
        p = lax.axis_index("tensor")
        rows = pl.ds(pl.multiple_of((2 * k + half) * self.chunk, self.chunk), self.chunk)
        q = p if half == 0 else self.n - 1 - p
        return q, p + 1 - 2 * half, p - 1 + 2 * half, rows

    def copy(self, half, k, kind, source, target, recv, device, rows):
        return pltpu.make_async_remote_copy(
            src_ref=source.at[rows, :], dst_ref=target.at[rows, :], send_sem=self.sems.at[kind, half, k],
            recv_sem=self.sems.at[recv, half, k], device_id={"tensor": device}, device_id_type=MESH)

    def inward_left(self, half, k):
        q, right, left, rows = self.at(half, k)
        return self.copy(half, k, 0, self.send, self.from_right, 2, left, rows)

    def inward_right(self, half, k):
        q, right, left, rows = self.at(half, k)
        return self.copy(half, k, 0, self.send, self.from_left, 1, right, rows)

    def outward_right(self, half, k):
        q, right, left, rows = self.at(half, k)
        return self.copy(half, k, 3, self.total, self.total, 5, right, rows)

    def outward_left(self, half, k):
        q, right, left, rows = self.at(half, k)
        return self.copy(half, k, 4, self.total, self.total, 5, left, rows)

    def edge(self, half, k):
        q = self.at(half, k)[0]

        @pl.when(q == self.n - 1)
        def _():
            self.inward_left(half, k).start()
        if self.owner > 0:
            @pl.when(q == 0)
            def _():
                self.inward_right(half, k).start()

    def mid(self, half, k):
        n, o = self.n, self.owner
        q, right, left, rows = self.at(half, k)
        if n - 1 - o > 1:
            @pl.when((q > o) & (q < n - 1))
            def _():
                self.inward_left(half, k).wait_recv()
                self.send[rows, :] = (self.send[rows, :].astype(F32) + self.from_right[rows, :].astype(F32)).astype(BF)
                self.inward_left(half, k).start()
        if o > 1:
            @pl.when((q < o) & (q > 0))
            def _():
                self.inward_right(half, k).wait_recv()
                self.send[rows, :] = (self.send[rows, :].astype(F32) + self.from_left[rows, :].astype(F32)).astype(BF)
                self.inward_right(half, k).start()

    def own(self, half, k):
        o = self.owner
        q, right, left, rows = self.at(half, k)

        @pl.when(q == o)
        def _():
            self.inward_left(half, k).wait_recv()
            total = self.send[rows, :].astype(F32) + self.from_right[rows, :].astype(F32)
            if o > 0:
                self.inward_right(half, k).wait_recv()
                total = total + self.from_left[rows, :].astype(F32)
            self.total[rows, :] = total.astype(BF)
            self.outward_right(half, k).start()
            if o > 0:
                self.outward_left(half, k).start()

    def forward(self, half, k):
        n, o = self.n, self.owner
        q = self.at(half, k)[0]

        @pl.when(q > o)
        def _():
            self.outward_right(half, k).wait_recv()

            @pl.when(q < n - 1)
            def _():
                self.outward_right(half, k).start()
        if o > 0:
            @pl.when(q < o)
            def _():
                self.outward_left(half, k).wait_recv()

                @pl.when(q > 0)
                def _():
                    self.outward_left(half, k).start()

    def drain(self, half, k):
        n, o = self.n, self.owner
        q = self.at(half, k)[0]

        @pl.when(q != o)
        def _():
            self.inward_left(half, k).wait_send()

        @pl.when((q >= o) & (q < n - 1))
        def _():
            self.outward_right(half, k).wait_send()
        if o > 0:
            @pl.when((q <= o) & (q > 0))
            def _():
                self.outward_left(half, k).wait_send()


def greet_line(n):
    p = lax.axis_index("tensor")
    barrier = pltpu.get_barrier_semaphore()

    @pl.when(p > 0)
    def _():
        pl.semaphore_signal(barrier, inc=1, device_id={"tensor": p - 1}, device_id_type=MESH)

    @pl.when(p < n - 1)
    def _():
        pl.semaphore_signal(barrier, inc=1, device_id={"tensor": p + 1}, device_id_type=MESH)

    inner = (p > 0) & (p < n - 1)

    @pl.when(inner)
    def _():
        pl.semaphore_wait(barrier, 2)

    @pl.when(jnp.logical_not(inner))
    def _():
        pl.semaphore_wait(barrier, 1)


def standardize(values):
    center = values - jnp.mean(values, axis=1, keepdims=True)
    rate = lax.rsqrt(jnp.mean(center * center, axis=1, keepdims=True) + eps_norm)
    return center * rate, rate


def norm_back(grad, unit, rate, gain):
    scaled = grad * gain
    return rate * (scaled - jnp.mean(scaled, axis=1, keepdims=True) - unit * jnp.mean(scaled * unit, axis=1, keepdims=True))


def middle_kernel(n, ctx, rows, side, norms, cot_hbm, up_hbm, down_hbm, outputs, d_first, d_ctx, g_up, g_down, g_out, g_norm,
                  cot, up, down, low, act, d_ffn, d_hid, d_br, unit, slope, d_sec, rates, sums, load_sems, *line_refs):
    R, D = rows.shape
    Wd = ctx.shape[1]
    chunk = R // (2 * ROUNDS)
    pair = 2 * chunk
    loads = [pltpu.make_async_copy(a, b, load_sems.at[i]) for i, (a, b) in
             enumerate([(up_hbm, up), (down_hbm, down), (cot_hbm, cot)])]
    for load in loads:
        load.start()
    lines = [Line(n, chunk, *line_refs[5 * i:5 * i + 5]) for i in range(3)]
    greet_line(n)
    sums[...] = jnp.zeros_like(sums)

    def add_sum(i, values):
        sums[8 * i:8 * i + 8, :] += jnp.sum(values.reshape(pair // 8, 8, D), axis=0)

    def pair_rows(k):
        return pl.ds(pl.multiple_of(k * pair, pair), pair)

    def open_first(k):
        r = pair_rows(k)
        lines[0].send[r, :] = dotf(ctx[r, :], side[:, :Wd], 1, 1).astype(BF)

    def first_to_second(k):
        r = pair_rows(k)
        u, rate = standardize(rows[r, :].astype(F32) + lines[0].total[r, :].astype(F32))
        unit[r, :] = u
        rates[r, :] = jnp.broadcast_to(rate, (pair, 128))
        nl = (u * norms[0:1, :] + norms[1:2, :]).astype(BF)
        low[r, :] = nl
        hidden = dotf(nl, up[...], 1, 0)
        half_cdf = 0.5 * (1.0 + lax.erf(hidden * 0.7071067811865476))
        slope[r, :] = half_cdf + hidden * (jnp.exp(-0.5 * hidden * hidden) * 0.3989422804014327)
        a = (hidden * half_cdf).astype(BF)
        act[r, :] = a
        lines[1].send[r, :] = dotf(a, down[...], 1, 1).astype(BF)

    def second_to_third(k):
        r = pair_rows(k)
        u, rate = standardize(unit[r, :] * norms[0:1, :] + norms[1:2, :] + lines[1].total[r, :].astype(F32))
        outputs[r, :] = (u * norms[2:3, :] + norms[3:4, :]).astype(BF)
        g = cot[r, :].astype(F32)
        add_sum(2, g * u)
        add_sum(3, g)
        ds = norm_back(g, u, rate, norms[2:3, :])
        d_sec[r, :] = ds
        dl = ds.astype(BF)
        d_ffn[r, :] = dl
        dh = (dotf(dl, down[...], 1, 0) * slope[r, :]).astype(BF)
        d_hid[r, :] = dh
        lines[2].send[r, :] = dotf(dh, up[...], 1, 1).astype(BF)

    def close_third(k):
        r = pair_rows(k)
        g = d_sec[r, :] + lines[2].total[r, :].astype(F32)
        u = unit[r, :]
        add_sum(0, g * u)
        add_sum(1, g)
        d1 = norm_back(g, u, rates[r, 0:1], norms[0:1, :])
        d_first[r, :] = d1
        db = d1.astype(BF)
        d_br[r, :] = db
        d_ctx[r, :] = dotf(db, side[:, :Wd], 1, 0).astype(BF)

    def weight_grad(out, left, right):
        width = min(256, D)

        def tile(i, _):
            c = pl.ds(pl.multiple_of(i * width, width), width)
            out[c, :] = dotf(left[:, c], right[...], 0, 0).astype(BF)
            return 0
        lax.fori_loop(0, D // width, tile, 0)

    def when_valid(t, lag, body):
        @pl.when((t >= lag) & (t < lag + ROUNDS))
        def _():
            body(t - lag)

    def both(stage):
        def run(k):
            stage(0, k)
            stage(1, k)
        return run

    def start(line, body):
        def run(k):
            body(k)
            line.edge(0, k)
            line.edge(1, k)
        return run

    def step(t, _):
        for i in (2, 1, 0):
            for lag, stage in ((8, lines[i].forward), (6, lines[i].own), (4, lines[i].mid)):
                when_valid(t, 8 * i + lag, both(stage))
        when_valid(t, 24, close_third)
        when_valid(t, 16, start(lines[2], second_to_third))
        when_valid(t, 8, start(lines[1], first_to_second))
        when_valid(t, 0, start(lines[0], open_first))

        @pl.when(t == 7)
        def _():
            for load in loads:
                load.wait()

        @pl.when(t == 16 + ROUNDS)
        def _():
            weight_grad(g_down, d_ffn, act)

        @pl.when(t == 17 + ROUNDS)
        def _():
            weight_grad(g_up, low, d_hid)
        return 0

    lax.fori_loop(0, ROUNDS + 24, step, 0)
    weight_grad(g_out, d_br, ctx)
    for i in range(4):
        g_norm[i:i + 1, :] = jnp.sum(sums[8 * i:8 * i + 8, :], axis=0, keepdims=True)
    g_norm[4:8, :] = jnp.zeros((4, D), F32)

    def finish(k, _):
        for line in lines:
            line.drain(0, k)
            line.drain(1, k)
        return 0
    lax.fori_loop(0, ROUNDS, finish, 0)


def middle(n, ctx, rows, side, norms, cot, up, down):
    R, D = rows.shape
    Wd, F = ctx.shape[1], up.shape[1]
    vmem, hbm = pl.BlockSpec(memory_space=pltpu.VMEM), pl.BlockSpec(memory_space=pl.ANY)
    line = [pltpu.VMEM((R, D), BF)] * 4 + [pltpu.SemaphoreType.DMA((6, 2, ROUNDS))]
    shape = jax.ShapeDtypeStruct
    return pl.pallas_call(
        partial(middle_kernel, n),
        in_specs=[vmem] * 4 + [hbm] * 3,
        out_specs=[vmem] * 7,
        out_shape=[shape((R, D), BF), shape((R, D), F32), shape((R, Wd), BF), shape((D, F), BF), shape((D, F), BF),
                   shape((D, Wd), BF), shape((8, D), F32)],
        scratch_shapes=[pltpu.VMEM((R, D), BF), pltpu.VMEM((D, F), BF), pltpu.VMEM((D, F), BF), pltpu.VMEM((R, D), BF),
                        pltpu.VMEM((R, F), BF), pltpu.VMEM((R, D), BF), pltpu.VMEM((R, F), BF), pltpu.VMEM((R, D), BF),
                        pltpu.VMEM((R, D), F32), pltpu.VMEM((R, F), F32), pltpu.VMEM((R, D), F32), pltpu.VMEM((R, 128), F32),
                        pltpu.VMEM((32, D), F32), pltpu.SemaphoreType.DMA((3,))] + line * 3,
        compiler_params=pltpu.CompilerParams(collective_id=1, has_side_effects=True),
        name="middle",
        cost_estimate=pl.CostEstimate(flops=12 * R * D * F, bytes_accessed=16 * R * D, transcendentals=2 * R * F),
    )(ctx, rows, side, norms, cot, up, down)


def plane_peers():
    s, c = lax.axis_index("shard"), lax.axis_index("context")
    near = [s, s + 1 - 2 * (s % 2), (s + 2) % 4, 3 - s]
    return near, c


def greet_plane():
    near, c = plane_peers()
    barrier = pltpu.get_barrier_semaphore()
    pl.semaphore_signal(barrier, inc=1, device_id={"context": 1 - c}, device_id_type=MESH)
    for j in (1, 2):
        pl.semaphore_signal(barrier, inc=1, device_id={"shard": near[j]}, device_id_type=MESH)
    pl.semaphore_wait(barrier, 3)


class Scatter:
    def __init__(self, mats, partner_in, acc, corner_in, came, sems, loads=None):
        self.mats, self.partner_in, self.acc, self.corner_in, self.came = mats, partner_in, acc, corner_in, came
        self.sems, self.loads = sems, loads
        self.own = corner_in.shape[1]

    def block(self, j):
        return pl.ds(j * self.own, self.own)

    def source(self, side, j, other):
        near, c = plane_peers()
        core = 1 - c if other else c
        return self.mats[side].at[pl.ds(pl.multiple_of((2 * near[j] + core) * self.own, self.own), self.own), :]

    def to_partner(self, side, j):
        c = lax.axis_index("context")
        return pltpu.make_async_remote_copy(
            src_ref=self.source(side, j, True), dst_ref=self.partner_in.at[side, self.block(j), :],
            send_sem=self.sems.at[0, side, j], recv_sem=self.sems.at[1, side, j], device_id={"context": 1 - c}, device_id_type=MESH)

    def load(self, side, j):
        return pltpu.make_async_copy(self.source(side, j, False), self.acc.at[side, self.block(j), :], self.loads.at[side, j])

    def hop(self, side, j, axis, target, kind):
        near, _ = plane_peers()
        return pltpu.make_async_remote_copy(
            src_ref=self.acc.at[side, self.block(j), :], dst_ref=target, send_sem=self.sems.at[2, side, kind],
            recv_sem=self.sems.at[3, side, kind], device_id={"shard": near[axis]}, device_id_type=MESH)

    def corner(self, side):
        return self.hop(side, 3, 1 + side, self.corner_in.at[side], 0)

    def early(self, side):
        return self.hop(side, 1 + side, 1 + side, self.came.at[side, 0], 1)

    def late(self, side):
        return self.hop(side, 2 - side, 2 - side, self.came.at[side, 1], 2)

    def begin(self, side):
        for j in (3, 1, 2, 0):
            self.to_partner(side, j).start()
            if self.loads is not None:
                self.load(side, j).start()

    def add_partner(self, side, j):
        self.to_partner(side, j).wait_recv()
        if self.loads is not None:
            self.load(side, j).wait()
            mine = self.acc[side, self.block(j), :]
        else:
            mine = self.source(side, j, False)[...]
        self.acc[side, self.block(j), :] = (mine.astype(F32) + self.partner_in[side, self.block(j), :].astype(F32)).astype(BF)

    def spread(self, side):
        self.add_partner(side, 3)
        self.corner(side).start()
        self.add_partner(side, 1 + side)
        self.early(side).start()
        self.add_partner(side, 2 - side)
        self.add_partner(side, 0)

    def turn(self, side):
        self.corner(side).wait_recv()
        b = self.block(2 - side)
        self.acc[side, b, :] = (self.acc[side, b, :].astype(F32) + self.corner_in[side].astype(F32)).astype(BF)
        self.late(side).start()

    def result(self, side):
        self.early(side).wait_recv()
        self.late(side).wait_recv()
        return (self.acc[side, self.block(0), :].astype(F32) + self.came[side, 0].astype(F32) + self.came[side, 1].astype(F32))

    def drain(self, side):
        for j in range(4):
            self.to_partner(side, j).wait_send()
        self.corner(side).wait_send()
        self.early(side).wait_send()
        self.late(side).wait_send()


def scatter_scratch(own, width, load):
    shapes = [pltpu.VMEM((2, 4 * own, width), BF), pltpu.VMEM((2, 4 * own, width), BF), pltpu.VMEM((2, own, width), BF),
              pltpu.VMEM((2, 2, own, width), BF), pltpu.SemaphoreType.DMA((4, 2, 4))]
    return shapes + ([pltpu.SemaphoreType.DMA((2, 4))] if load else [])


def attend_back_scatter_kernel(*refs, scale):
    ins, (g_up, g_down), outs, (o_up, o_down), scratch, shared = refs[:7], refs[7:9], refs[9:14], refs[14:16], refs[16:19], refs[19:]
    job = Scatter((g_up, g_down), *shared)
    step, last = pl.program_id(0), pl.num_programs(0) - 1

    @pl.when(step == 0)
    def _():
        greet_plane()
        job.begin(0)
        job.begin(1)

    def between(half):
        if half == 0:
            @pl.when(step == 0)
            def _():
                job.spread(0)
                job.spread(1)
        else:
            @pl.when(step == 0)
            def _():
                job.turn(0)
                job.turn(1)

    attend_back_kernel(*ins, *outs, *scratch, scale=scale, between=between)

    @pl.when(step == last)
    def _():
        o_up[...] = job.result(0)
        o_down[...] = job.result(1).T
        job.drain(0)
        job.drain(1)


def attend_back_scatter(q, k, v, kd, pq, p, dc, g_up, g_down, scale):
    S, L, Wd = q.shape
    T = k.shape[1]
    W = kd.shape[0]
    D, F = g_up.shape
    own, pairs = D // 8, Wd // 128
    row = lambda n: pl.BlockSpec((1, n, 128), lambda h, s: (s, 0, h))
    tab = pl.BlockSpec((W, 128), lambda h, s: (0, h))
    hbm = pl.BlockSpec(memory_space=pl.ANY)
    fixed = lambda *shape: pl.BlockSpec(shape, lambda h, s: (0, 0))
    return pl.pallas_call(
        partial(attend_back_scatter_kernel, scale=scale), grid=(pairs, S),
        in_specs=[row(L), row(T), row(T), tab, tab, pl.BlockSpec((1, 2, L, T), lambda h, s: (s, h, 0, 0)), row(L), hbm, hbm],
        out_specs=[row(L), row(T), row(T), tab, tab, fixed(own, F), fixed(F, own)],
        out_shape=[jax.ShapeDtypeStruct((S, n, Wd), BF) for n in (L, T, T)] + [jax.ShapeDtypeStruct((W, Wd), F32)] * 2
        + [jax.ShapeDtypeStruct((own, F), F32), jax.ShapeDtypeStruct((F, own), F32)],
        scratch_shapes=[pltpu.VMEM((L, T), BF), pltpu.VMEM((L, T), BF), pltpu.VMEM((T, HD), F32)] + scatter_scratch(own, F, True),
        compiler_params=pltpu.CompilerParams(collective_id=3, has_side_effects=True),
        name="attend_back",
        cost_estimate=pl.CostEstimate(flops=int(32 * S * L * T * Wd), bytes_accessed=int(S * L * T * Wd // HD * 4), transcendentals=0),
    )(q, k, v, kd, pq, p, dc, g_up, g_down)


def tail_kernel(n, dq, dk, dv, wqkv, rows, d_first, side, to_row, from_row, dkd, dpq, g_out, g_norm,
                grad_in, o_q, o_k, o_v, o_out, o_pos, o_norm,
                k_in, v_in, dqkv, d_pos, g_left, g_right, norm_in, swap_sems, norm_sems, *refs):
    L, Wd = dq.shape
    D, B = side.shape[0], side.shape[1] - Wd
    W = to_row.shape[1]
    own = D // 8
    chunk = L // (2 * ROUNDS)
    pair = 2 * chunk
    line = Line(n, chunk, *refs[:5])
    small = Line(n, own // 2, *refs[5:10])
    job = Scatter((g_left, g_right), *refs[10:])
    near, c = plane_peers()
    p = lax.axis_index("tensor")
    barrier = pltpu.get_barrier_semaphore()
    for j in range(4):
        for core in (c, 1 - c):
            if j > 0 or core is not c:
                pl.semaphore_signal(barrier, inc=1, device_id={"shard": near[j], "context": core}, device_id_type=MESH)

    @pl.when(p > 0)
    def _():
        pl.semaphore_signal(barrier, inc=1, device_id={"tensor": p - 1}, device_id_type=MESH)

    @pl.when(p < n - 1)
    def _():
        pl.semaphore_signal(barrier, inc=1, device_id={"tensor": p + 1}, device_id_type=MESH)
    inner = (p > 0) & (p < n - 1)

    @pl.when(inner)
    def _():
        pl.semaphore_wait(barrier, 9)

    @pl.when(jnp.logical_not(inner))
    def _():
        pl.semaphore_wait(barrier, 8)

    def swap(i, source, target):
        part = pl.ds(pl.multiple_of((1 - c) * L, L), L)
        return pltpu.make_async_remote_copy(src_ref=source.at[part, :], dst_ref=target, send_sem=swap_sems.at[0, i],
                                            recv_sem=swap_sems.at[1, i], device_id={"context": 1 - c}, device_id_type=MESH)
    swaps = [swap(0, dk, k_in), swap(1, dv, v_in)]
    for s in swaps:
        s.start()
    pieces = []
    for j in range(4):
        for other in range(2):
            core = c if other == 0 else 1 - c
            if j == 0 and other == 0:
                continue
            i = 2 * j + other
            lanes = pl.ds(pl.multiple_of((2 * near[j] + core) * own, own), own)
            pieces.append(pltpu.make_async_remote_copy(
                src_ref=g_norm.at[:, lanes], dst_ref=norm_in.at[i], send_sem=norm_sems.at[0, i], recv_sem=norm_sems.at[1, i],
                device_id={"shard": near[j], "context": core}, device_id_type=MESH))
    for piece in pieces:
        piece.start()

    ids = lax.broadcasted_iota(jnp.int32, (B, W), 0)
    d_pos[:, :Wd] = dotf((ids == from_row[...]).astype(F32).astype(BF), dpq[...].astype(BF), 1, 0).astype(BF)
    d_pos[:, Wd:] = dotf((ids == to_row[...]).astype(F32).astype(BF), dkd[...].astype(BF), 1, 0).astype(BF)
    g_right[:, :Wd] = g_out[...]
    width = 256

    def right_tile(i, _):
        r = pl.ds(pl.multiple_of(i * width, width), width)
        g_right[r, Wd:] = dotf(wqkv[r, :2 * Wd], d_pos[...], 1, 1).astype(BF)
        return 0
    lax.fori_loop(0, D // width, right_tile, 0)
    job.begin(1)
    here = pl.ds(pl.multiple_of(c * L, L), L)
    dqkv[:, :Wd] = dq[...]
    for s, mine, got, at in ((swaps[0], dk, k_in, Wd), (swaps[1], dv, v_in, 2 * Wd)):
        s.wait_recv()
        dqkv[:, at:at + Wd] = (mine[here, :].astype(F32) + got[...].astype(F32)).astype(BF)

    def pair_rows(k):
        return pl.ds(pl.multiple_of(k * pair, pair), pair)

    def produce(k, _):
        r = pair_rows(k)
        line.send[r, :] = dotf(dqkv[r, :], wqkv[...], 1, 1).astype(BF)
        line.edge(0, k)
        line.edge(1, k)
        return 0
    lax.fori_loop(0, ROUNDS, produce, 0)

    def left_tile(i, _):
        r = pl.ds(pl.multiple_of(i * width, width), width)
        g = dotf(rows[:, r], dqkv[...], 0, 0)
        g_left[r, :2 * Wd] = (g[:, :2 * Wd] + dotf(side[r, Wd:], d_pos[...], 1, 0)).astype(BF)
        g_left[r, 2 * Wd:] = g[:, 2 * Wd:].astype(BF)
        return 0
    lax.fori_loop(0, D // width, left_tile, 0)
    job.begin(0)
    job.spread(1)

    def step(t, _):
        for lag, stage in ((4, line.forward), (2, line.own), (0, line.mid)):
            @pl.when((t >= lag) & (t < lag + ROUNDS))
            def _():
                stage(0, t - lag)
                stage(1, t - lag)

        @pl.when((t >= 4) & (t < 4 + ROUNDS))
        def _():
            r = pair_rows(t - 4)
            grad_in[r, :] = (d_first[r, :] + line.total[r, :].astype(F32)).astype(BF)

        @pl.when(t == 0)
        def _():
            job.spread(0)

        @pl.when(t == 2)
        def _():
            job.turn(1)
            job.turn(0)

        @pl.when(t == 6)
        def _():
            right = job.result(1)
            o_out[...] = right[:, :Wd].T
            small.send[...] = right[:, Wd:].astype(BF)
            small.edge(0, 0)
            small.edge(1, 0)

        @pl.when(t == 7)
        def _():
            left = job.result(0)
            o_q[...] = left[:, :Wd]
            o_k[...] = left[:, Wd:2 * Wd]
            o_v[...] = left[:, 2 * Wd:]

        for at, stage in ((8, small.mid), (9, small.own), (11, small.forward)):
            @pl.when(t == at)
            def _():
                stage(0, 0)
                stage(1, 0)
        return 0
    lax.fori_loop(0, ROUNDS + 4, step, 0)
    o_pos[...] = small.total[...].astype(F32).T
    lanes = pl.ds(pl.multiple_of((2 * near[0] + c) * own, own), own)
    total = g_norm[:, lanes]
    for piece in pieces:
        piece.wait_recv()
    for i in range(1, 8):
        total = total + norm_in[i]
    o_norm[...] = total

    def finish(k, _):
        line.drain(0, k)
        line.drain(1, k)
        return 0
    lax.fori_loop(0, ROUNDS, finish, 0)
    small.drain(0, 0)
    small.drain(1, 0)
    job.drain(0)
    job.drain(1)
    for copy in swaps + pieces:
        copy.wait_send()


def tail(n, dq, dk, dv, wqkv, rows, d_first, side, to_row, from_row, dkd, dpq, g_out, g_norm):
    L, Wd = dq.shape
    D, B = side.shape[0], side.shape[1] - Wd
    own = D // 8
    vmem = pl.BlockSpec(memory_space=pltpu.VMEM)
    shape = jax.ShapeDtypeStruct
    line = [pltpu.VMEM((L, D), BF)] * 4 + [pltpu.SemaphoreType.DMA((6, 2, ROUNDS))]
    small = [pltpu.VMEM((own, B), BF)] * 4 + [pltpu.SemaphoreType.DMA((6, 2, 1))]
    return pl.pallas_call(
        partial(tail_kernel, n),
        in_specs=[vmem] * 13, out_specs=[vmem] * 7,
        out_shape=[shape((L, D), BF)] + [shape((own, Wd), F32)] * 3 + [shape((Wd, own), F32), shape((B, own), F32), shape((8, own), F32)],
        scratch_shapes=[pltpu.VMEM((L, Wd), BF), pltpu.VMEM((L, Wd), BF), pltpu.VMEM((L, 3 * Wd), BF), pltpu.VMEM((B, 2 * Wd), BF),
                        pltpu.VMEM((D, 3 * Wd), BF), pltpu.VMEM((D, Wd + B), BF), pltpu.VMEM((8, 8, own), F32),
                        pltpu.SemaphoreType.DMA((2, 2)), pltpu.SemaphoreType.DMA((2, 8))] + line + small
        + scatter_scratch(own, 3 * Wd, False),
        compiler_params=pltpu.CompilerParams(collective_id=4, has_side_effects=True),
        name="tail",
        cost_estimate=pl.CostEstimate(flops=8 * L * D * 3 * Wd, bytes_accessed=16 * L * D, transcendentals=0),
    )(dq, dk, dv, wqkv, rows, d_first, side, to_row, from_row, dkd, dpq, g_out, g_norm)


class Gather:
    def __init__(self, mats, sems, first=None):
        self.mats, self.sems, self.first = mats, sems, first
        self.near, self.core = plane_peers()
        self.own = mats[0].shape[0] // 8

    def rows(self, j, other=False):
        core = 1 - self.core if other else self.core
        return pl.ds(pl.multiple_of((2 * self.near[j] + core) * self.own, self.own), self.own)

    def copy(self, side, rows, kind, i, device, first=False):
        block = self.mats[side].at[rows, :]
        return pltpu.make_async_remote_copy(
            src_ref=self.first[side] if first and self.first is not None else block, dst_ref=block,
            send_sem=self.sems.at[0, kind, side, i], recv_sem=self.sems.at[1, kind, side, i], device_id=device, device_id_type=MESH)

    def direct(self, side, axis, receive=False):
        return self.copy(side, self.rows(axis if receive else 0), 0, axis, {"shard": self.near[axis]}, not receive)

    def relay(self, side, receive=False):
        return self.copy(side, self.rows(3 if receive else 1 + side), 0, 0, {"shard": self.near[2 - side]})

    def partner(self, side, j, receive=False):
        return self.copy(side, self.rows(j, receive), 1, j, {"context": 1 - self.core}, j == 0 and not receive)

    def begin(self):
        for a in (0, 1):
            self.direct(a, 1 + a).start()
        for a in (0, 1):
            self.direct(a, 2 - a).start()
        for a in (0, 1):
            self.partner(a, 0).start()

    def turn(self):
        for a in (0, 1):
            self.direct(a, 1 + a, True).wait_recv()
            self.relay(a).start()
            self.partner(a, 1 + a).start()

    def share(self):
        for a in (0, 1):
            self.direct(a, 2 - a, True).wait_recv()
            self.partner(a, 2 - a).start()

    def corner(self):
        for a in (0, 1):
            self.relay(a, True).wait_recv()
            self.partner(a, 3).start()

    def close(self):
        for a in (0, 1):
            for j in range(4):
                self.partner(a, j, True).wait_recv()
        for a in (0, 1):
            self.direct(a, 1).wait_send()
            self.direct(a, 2).wait_send()
            self.relay(a).wait_send()
            for j in range(4):
                self.partner(a, j).wait_send()


def open_kernel(x, w_q, w_k, w_v, w_o, pos, norms, to_row, from_row, q, k, v, kd, pq, wqkv, side, all_norms,
                x_in, pos_qk, swap_sems, norm_sems, sems):
    L, D = x.shape
    own, Wd = w_q.shape
    B, W = pos.shape[0], to_row.shape[1]
    near, c = plane_peers()
    mine = pl.ds(pl.multiple_of((2 * near[0] + c) * own, own), own)
    wqkv[mine, :Wd] = w_q[...]
    wqkv[mine, Wd:2 * Wd] = w_k[...]
    wqkv[mine, 2 * Wd:] = w_v[...]
    side[mine, :Wd] = w_o[...].T
    side[mine, Wd:] = pos[...].T
    all_norms[:, mine] = norms[...]
    peers = [(j, other) for j in range(4) for other in (0, 1) if j or other]
    device = lambda j, other: {"shard": near[j], "context": 1 - c if other else c}
    barrier = pltpu.get_barrier_semaphore()
    for j, other in peers:
        pl.semaphore_signal(barrier, inc=1, device_id=device(j, other), device_id_type=MESH)
    pl.semaphore_wait(barrier, 7)
    job = Gather((wqkv, side), sems)
    job.begin()
    swap = pltpu.make_async_remote_copy(src_ref=x, dst_ref=x_in, send_sem=swap_sems.at[0], recv_sem=swap_sems.at[1],
                                        device_id={"context": 1 - c}, device_id_type=MESH)
    swap.start()

    def piece(j, other, receive):
        core = 1 - c if other and receive else c
        lanes = pl.ds(pl.multiple_of((2 * near[j if receive else 0] + core) * own, own), own)
        return pltpu.make_async_remote_copy(
            src_ref=norms, dst_ref=all_norms.at[:, lanes], send_sem=norm_sems.at[0, 2 * j + other],
            recv_sem=norm_sems.at[1, 2 * j + other], device_id=device(j, other), device_id_type=MESH)
    for j, other in peers:
        piece(j, other, False).start()
    job.turn()
    job.share()
    swap.wait_recv()
    job.corner()
    job.close()
    tile = min(256, L)

    def project(i, _):
        r = pl.ds(pl.multiple_of(i * tile, tile), tile)
        here = pl.ds(pl.multiple_of(c * L + i * tile, tile), tile)
        there = pl.ds(pl.multiple_of((1 - c) * L + i * tile, tile), tile)
        out = dotf(x[r, :], wqkv[...], 1, 0).astype(BF)
        q[r, :] = out[:, :Wd]
        k[here, :] = out[:, Wd:2 * Wd]
        v[here, :] = out[:, 2 * Wd:]
        out = dotf(x_in[r, :], wqkv[:, Wd:], 1, 0).astype(BF)
        k[there, :] = out[:, :Wd]
        v[there, :] = out[:, Wd:]
        return 0
    lax.fori_loop(0, L // tile, project, 0)
    pos_qk[...] = dotf(side[:, Wd:], wqkv[:, :2 * Wd], 0, 0).astype(BF)
    ids = lax.broadcasted_iota(jnp.int32, (B, 256), 0)

    def table(i, _):
        r = pl.ds(pl.multiple_of(i * 256, 256), 256)
        kd[r, :] = dotf((ids == to_row[:, r]).astype(F32).astype(BF), pos_qk[:, Wd:], 0, 0).astype(BF)
        pq[r, :] = dotf((ids == from_row[:, r]).astype(F32).astype(BF), pos_qk[:, :Wd], 0, 0).astype(BF)
        return 0
    lax.fori_loop(0, W // 256, table, 0)
    for j, other in peers:
        piece(j, other, True).wait_recv()
    for j, other in peers:
        piece(j, other, False).wait_send()
    swap.wait_send()


def open_gather(x, w_q, w_k, w_v, w_o, pos, norms, to_row, from_row):
    L, D = x.shape
    own, Wd = w_q.shape
    B, W = pos.shape[0], to_row.shape[1]
    T = W - L
    vmem = pl.BlockSpec(memory_space=pltpu.VMEM)
    shape = jax.ShapeDtypeStruct
    return pl.pallas_call(
        open_kernel, in_specs=[vmem] * 9, out_specs=[vmem] * 8,
        out_shape=[shape((L, Wd), BF), shape((T, Wd), BF), shape((T, Wd), BF), shape((W, Wd), BF), shape((W, Wd), BF),
                   shape((D, 3 * Wd), BF), shape((D, Wd + B), BF), shape((8, D), F32)],
        scratch_shapes=[pltpu.VMEM((L, D), BF), pltpu.VMEM((B, 2 * Wd), BF), pltpu.SemaphoreType.DMA((2,)),
                        pltpu.SemaphoreType.DMA((2, 8)), pltpu.SemaphoreType.DMA((2, 2, 2, 4))],
        compiler_params=pltpu.CompilerParams(collective_id=5, has_side_effects=True),
        name="open",
        cost_estimate=pl.CostEstimate(flops=10 * L * D * Wd, bytes_accessed=8 * L * D, transcendentals=0),
    )(x, w_q, w_k, w_v, w_o, pos, norms, to_row, from_row)


def attend_gather_kernel(*refs, scale):
    ins, (w_up, w_down), outs, mats, st, turned, sems, local_sems = refs[:7], refs[7:9], refs[9:11], refs[11:13], *refs[13:]
    step, last = pl.program_id(1), pl.num_programs(1) - 1
    job = Gather(mats, sems, first=(w_up, turned))
    keep = [pltpu.make_async_copy(a, m.at[job.rows(0), :], local_sems.at[i])
            for i, (a, m) in enumerate(zip((w_up, turned), mats))]

    @pl.when(step == 0)
    def _():
        turned[...] = w_down[...].T
        greet_plane()
        job.begin()
        for copy in keep:
            copy.start()

    def between(half):
        if half == 1:
            @pl.when(step == 0)
            def _():
                job.turn()
        else:
            @pl.when(step == last)
            def _():
                job.share()

    attend_kernel(*ins, *outs, st, scale=scale, between=between)

    @pl.when(step == last)
    def _():
        job.corner()
        job.close()
        for copy in keep:
            copy.wait()


def attend_gather(q, k, v, kd, pq, sq, sk, w_up, w_down, scale):
    S, L, Wd = q.shape
    T = k.shape[1]
    W = kd.shape[0]
    own, F = w_up.shape
    pairs = Wd // 128
    row = lambda n: pl.BlockSpec((1, n, 128), lambda s, h: (s, 0, h))
    tab = pl.BlockSpec((W, 128), lambda s, h: (0, h))
    vmem, hbm = pl.BlockSpec(memory_space=pltpu.VMEM), pl.BlockSpec(memory_space=pl.ANY)
    shape = jax.ShapeDtypeStruct
    return pl.pallas_call(
        partial(attend_gather_kernel, scale=scale), grid=(S, pairs),
        in_specs=[row(L), row(T), row(T), tab, tab, pl.BlockSpec((1, L, 1), lambda s, h: (s, 0, 0)),
                  pl.BlockSpec((1, 1, T), lambda s, h: (s, 0, 0)), vmem, vmem],
        out_specs=[row(L), pl.BlockSpec((1, 2, L, T), lambda s, h: (s, h, 0, 0)), hbm, hbm],
        out_shape=[shape((S, L, Wd), BF), shape((S, Wd // HD, L, T), F32), shape((8 * own, F), BF), shape((8 * own, F), BF)],
        scratch_shapes=[pltpu.VMEM((L, T), F32), pltpu.VMEM((own, F), BF), pltpu.SemaphoreType.DMA((2, 2, 2, 4)),
                        pltpu.SemaphoreType.DMA((2,))],
        compiler_params=pltpu.CompilerParams(collective_id=6, has_side_effects=True),
        name="attend",
        cost_estimate=pl.CostEstimate(flops=int(16 * S * L * T * Wd), bytes_accessed=int(S * L * T * Wd // HD * 4),
                                      transcendentals=S * L * T * Wd // HD),
    )(q, k, v, kd, pq, sq, sk, w_up, w_down)


def split_columns(packed, widths):
    at, out = 0, []
    for width in widths:
        out.append(packed[:, at:at + width])
        at += width
    return out


def local(inputs, cotangent, segments, buckets, w_query, w_key, w_value, w_output, w_up, w_down,
          positions, gain_attn, bias_attn, gain_ffn, bias_ffn):
    S, L, D = inputs.shape
    T = segments.shape[1]
    Wd = w_query.shape[1]
    F = w_up.shape[1]
    B = positions.shape[0]
    scale = 1.0 / math.sqrt(3 * HD)
    first = lax.axis_index("context") * L
    W = T + L
    own = w_query.shape[0]
    flipped = jnp.concatenate([buckets[::-1], buckets[:1]])
    to = lax.dynamic_slice_in_dim(flipped, T - L - first, W, 0)
    fro = lax.dynamic_slice_in_dim(flipped, first, W, 0)
    seg_here = lax.dynamic_slice_in_dim(segments, first, L, 1)[:, :, None]
    seg_row = segments[:, None, :]
    rows = inputs.reshape(S * L, D)
    square = (lax.axis_size("shard"), lax.axis_size("context"), S, own * 8, 3 * Wd) == (4, 2, 1, D, Wd + B)
    norms = jnp.stack([gain_attn, bias_attn, gain_ffn, bias_ffn]).astype(F32)
    if square:
        q, k, v, kd, pq, wqkv, side, norms = open_gather(
            rows, w_query, w_key, w_value, w_output, positions, jnp.pad(norms, ((0, 4), (0, 0))), to[None], fro[None])
        q, k, v = q[None], k[None], v[None]
        ctx, probs, up, down_t = attend_gather(q, k, v, kd, pq, seg_here, seg_row, w_up, w_down, scale)
    else:
        norms = jnp.pad(norms.astype(BF).T, ((0, 0), (0, 124)))
        pack = jnp.concatenate([w_query, w_key, w_value, w_output.T, positions.T, norms], axis=1)
        pack = lax.all_gather(pack, BOTH, axis=0, tiled=True)
        wqkv, side, norms = split_columns(pack, (3 * Wd, Wd + B, 128))
        ffn = lax.all_gather(jnp.concatenate([w_up, w_down.T], axis=1), BOTH, axis=0, tiled=True)
        up, down_t = split_columns(ffn, (F, F))
        norms = jnp.pad(norms[:, :4].astype(F32).T, ((0, 4), (0, 0)))
        qkv = dotf(rows, wqkv, 1, 0).astype(BF)
        q, k, v = [x.reshape(S, L, Wd) for x in split_columns(qkv, (Wd, Wd, Wd))]
        k, v = split_last(lax.all_gather(jnp.concatenate([k, v], axis=2), "context", axis=1, tiled=True), Wd)
        pos_qk = dotf(side[:, Wd:], wqkv[:, :2 * Wd], 0, 0).astype(BF)
        ids = jnp.arange(B, dtype=jnp.int32)
        pick_to = (to[:, None] == ids[None]).astype(BF)
        pick_from = (fro[:, None] == ids[None]).astype(BF)
        kd = dotf(pick_to, pos_qk[:, Wd:], 1, 0).astype(BF)
        pq = dotf(pick_from, pos_qk[:, :Wd], 1, 0).astype(BF)
        ctx, probs = attend(q, k, v, kd, pq, seg_here, seg_row, scale)
    ctx_rows = ctx.reshape(S * L, Wd)
    outputs, d_first, d_ctx, g_up, g_down_t, g_out_t, g_norm = middle(
        lax.axis_size("tensor"), ctx_rows, rows, side, norms, cotangent.reshape(S * L, D), up, down_t)
    outputs = outputs.reshape(inputs.shape)
    f = lambda x: x.astype(F32)
    if square:
        dq, dk, dv, dkd, dpq, g_up, g_down = attend_back_scatter(q, k, v, kd, pq, probs, d_ctx.reshape(S, L, Wd), g_up, g_down_t, scale)
        grad_inputs, g_q, g_k, g_v, g_o, g_p, g_n = tail(
            lax.axis_size("tensor"), dq[0], dk[0], dv[0], wqkv, rows, d_first, side, to[None], fro[None], dkd, dpq, g_out_t, g_norm)
        return (outputs, grad_inputs.reshape(inputs.shape), g_q, g_k, g_v, g_o, g_up, g_down, g_p, g_n[0], g_n[1], g_n[2], g_n[3])
    scatter = partial(lax.psum_scatter, axis_name=BOTH, scatter_dimension=0, tiled=True)
    g_ffn = scatter(jnp.concatenate([g_up, g_down_t], axis=1))
    dq, dk, dv, dkd, dpq = attend_back(q, k, v, kd, pq, probs, d_ctx.reshape(S, L, Wd), scale)
    dkv = lax.psum_scatter(jnp.concatenate([dk, dv], axis=2), "context", scatter_dimension=1, tiled=True)
    dqkv = jnp.concatenate([dq, dkv], axis=2).reshape(S * L, 3 * Wd)
    d_in = lax.psum(dotf(dqkv, wqkv, 1, 1).astype(BF), "tensor").astype(F32)
    grad_inputs = (d_first + d_in).astype(BF).reshape(inputs.shape)
    d_pos_key = dotf(pick_to, dkd.astype(BF), 0, 0)
    d_pos_query = dotf(pick_from, dpq.astype(BF), 0, 0)
    d_pos = jnp.concatenate([d_pos_query, d_pos_key], axis=1).astype(BF)
    g_qkv = dotf(rows, dqkv, 0, 0)
    g_pos_t = dotf(wqkv[:, :2 * Wd], d_pos, 1, 1)
    g_qk = g_qkv[:, :2 * Wd] + dotf(side[:, Wd:], d_pos, 1, 0)
    g_norm = jnp.pad(g_norm.T, ((0, 0), (0, 120)))
    pack = jnp.concatenate([x.astype(BF) for x in (g_qk, g_qkv[:, 2 * Wd:], g_out_t, g_pos_t, g_norm)], axis=1)
    g_q, g_k, g_v, g_o, g_p, g_n = split_columns(scatter(pack), (Wd, Wd, Wd, Wd, B, 128))
    g_p = lax.psum(g_p, "tensor")
    return (outputs, grad_inputs, f(g_q), f(g_k), f(g_v), f(g_o).T, f(g_ffn[:, :F]), f(g_ffn[:, F:]).T, f(g_p).T,
            f(g_n[:, 0]), f(g_n[:, 1]), f(g_n[:, 2]), f(g_n[:, 3]))


def split_last(packed, width):
    return packed[..., :width], packed[..., width:]


def solution(mesh):
    P = jax.sharding.PartitionSpec
    act, row, col, vec = P("shard", "context", None), P(BOTH, "tensor"), P("tensor", BOTH), P(BOTH)
    return jax.shard_map(local, mesh=mesh,
        in_specs=(act, act, P("shard", None), P(), row, row, row, col, row, col, P(None, BOTH), vec, vec, vec, vec),
        out_specs=(act, act, row, row, row, col, row, col, P(None, BOTH), vec, vec, vec, vec),
        check_vma=False)
```
